16 devices in a mesh: rep: 1, dp: 16 (over x, y, z, core).
Axes of the slice: x: 2, y: 2, z: 2, core: 2. Of those that a mesh axis runs over, the one named last changes fastest.
Arguments:
- x: bfloat16 [16, 2048, 1024], P(('rep', 'dp'))
- dy: bfloat16 [16, 2048, 1024], P(('rep', 'dp'))
- w_gate: bfloat16 [2, 1024, 4096], P(None, 'dp')
- w_up: bfloat16 [2, 1024, 4096], P(None, 'dp')
- w_down: bfloat16 [2, 4096, 1024], P(None, 'dp')
- m_w_gate: float32 [2, 1024, 4096], P(None, 'dp')
- m_w_up: float32 [2, 1024, 4096], P(None, 'dp')
- m_w_down: float32 [2, 4096, 1024], P(None, 'dp')
- v_w_gate: float32 [2, 1024, 4096], P(None, 'dp')
- v_w_up: float32 [2, 1024, 4096], P(None, 'dp')
- v_w_down: float32 [2, 4096, 1024], P(None, 'dp')
Outputs:
- output 1: bfloat16 [2, 1024, 4096], P('rep', 'dp')
- output 2: bfloat16 [2, 1024, 4096], P('rep', 'dp')
- output 3: bfloat16 [2, 4096, 1024], P('rep', 'dp')
- output 4: float32 [2, 1024, 4096], P('rep', 'dp')
- output 5: float32 [2, 1024, 4096], P('rep', 'dp')
- output 6: float32 [2, 4096, 1024], P('rep', 'dp')
- output 7: float32 [2, 1024, 4096], P('rep', 'dp')
- output 8: float32 [2, 1024, 4096], P('rep', 'dp')
- output 9: float32 [2, 4096, 1024], P('rep', 'dp')
All inputs are finite; a program needn't handle non-finite values.
Results may differ from the reference program's by a relative error of at most 0.0224.
Values are sent between devices in bfloat16 or wider.
A program may use at most 2 GiB of HBM per device.

```python
import jax
import jax.numpy as jnp
from jax import lax

SEQUENCES = 16
TOKENS = 2048
D = 1024
FF = 4096
LAYERS = 2
NAMES = ("w_gate", "w_up", "w_down")
SHAPES = {"w_gate": (LAYERS, D, FF), "w_up": (LAYERS, D, FF), "w_down": (LAYERS, FF, D)}


def bump(key, n, height):
    away = (jnp.arange(n, dtype=jnp.int32) - jax.random.randint(key, (), 0, n, jnp.int32)) % n
    return jnp.where(away < n // 8, height, 1.0)


def together(key, own, strength):
    shared = jax.random.normal(key, own.shape[1:], jnp.float32)
    return (own + strength * shared) * lax.rsqrt(1 + strength * strength)


def setup_inputs(seed: int = 0, part: int = 0) -> dict:
    kx, kdy, ka, kb, kz, kf, kh, kl, *keys = jax.random.split(jax.random.key(seed), 8 + 3 * len(NAMES))
    kx, kdy, ka, kb = (jax.random.fold_in(k, part) for k in (kx, kdy, ka, kb))
    kw, km, kv = (keys[i::3] for i in range(3))
    shape = (SEQUENCES, TOKENS, D)
    much_x, much_dy = jax.random.uniform(kz, (2,), jnp.float32, 0.0, 1.0)
    loud = 2.0 ** jax.random.uniform(jax.random.fold_in(kz, 1), (), jnp.float32, -1.0, 2.0)
    layers = 2.0 ** jax.random.uniform(kl, (LAYERS, 1, 1), jnp.float32, -1.0, 1.0)
    x = together(ka, jax.random.normal(kx, shape, jnp.float32), much_x) * bump(kf, D, 4.0)
    dy = together(kb, jax.random.normal(kdy, shape, jnp.float32), much_dy)
    drawn = {"x": x.astype(jnp.bfloat16), "dy": (loud * dy * (SEQUENCES * TOKENS) ** -0.5).astype(jnp.bfloat16)}
    for key, name in zip(kw, NAMES, strict=True):
        w = jax.random.normal(key, SHAPES[name], jnp.float32) * SHAPES[name][1] ** -0.5
        drawn[name] = (w * {"w_gate": 1.0, "w_up": bump(kh, FF, 4.0), "w_down": layers}[name]).astype(jnp.bfloat16)
    for key, name in zip(km, NAMES, strict=True):
        drawn[f"m_{name}"] = 0.1 * jax.random.normal(key, SHAPES[name], jnp.float32)
    for key, name in zip(kv, NAMES, strict=True):
        drawn[f"v_{name}"] = jax.random.uniform(key, SHAPES[name], jnp.float32, 0.005, 0.015)
    return drawn


def matmul(a, w):
    return jnp.dot(a, w, preferred_element_type=jnp.float32).astype(jnp.bfloat16)


def normed(h):
    wide = h.astype(jnp.float32)
    scale = lax.rsqrt(jnp.mean(wide**2, -1, keepdims=True) + 1e-6)
    return (wide * scale).astype(jnp.bfloat16)


def layer(h, w):
    a = normed(h)
    gate = jnp.dot(a, w["w_gate"], preferred_element_type=jnp.float32)
    up = jnp.dot(a, w["w_up"], preferred_element_type=jnp.float32)
    return h + matmul((jax.nn.silu(gate) * up).astype(jnp.bfloat16), w["w_down"])


def adamw(w, m, v, g):
    m = 0.9 * m + 0.1 * g
    v = 0.95 * v + 0.05 * g * g
    step = m * lax.rsqrt(v + 1e-8) + 0.1 * w
    return (w - 0.02 * step).astype(jnp.bfloat16), m, v


def clipped(gradients, sum_of_squares, count):
    factor = jnp.minimum(1.0, 0.5 * lax.rsqrt(sum_of_squares / count + 1e-30))
    return [g * factor for g in gradients]


def stack(weights, h):
    return lax.scan(lambda h, w: (layer(h, w), None), h, weights)[0]


def reference(x, dy, w_gate, w_up, w_down, m_w_gate, m_w_up, m_w_down, v_w_gate, v_w_up, v_w_down):
    weights = dict(zip(NAMES, (w_gate, w_up, w_down), strict=True))

    def take(so_far, sequence):
        h, by_y = sequence
        _, back = jax.vjp(lambda w: stack(w, h), weights)
        return jax.tree.map(lambda total, term: total + term.astype(jnp.float32), so_far, back(by_y)[0]), None

    none_yet = {name: jnp.zeros(w.shape, jnp.float32) for name, w in weights.items()}
    by_weights, _ = lax.scan(take, none_yet, (x, dy))
    gradients = [by_weights[name].astype(jnp.bfloat16).astype(jnp.float32) for name in NAMES]
    gradients = clipped(gradients, sum(jnp.sum(g * g) for g in gradients), sum(g.size for g in gradients))
    new = [
        adamw(w.astype(jnp.float32), m, v, g)
        for w, m, v, g in zip((w_gate, w_up, w_down), (m_w_gate, m_w_up, m_w_down), (v_w_gate, v_w_up, v_w_down), gradients, strict=True)
    ]
    return tuple(one[which] for which in range(3) for one in new)
```

```python
import functools

import jax
import jax.numpy as jnp
from jax import lax
from jax.experimental import pallas as pl
from jax.experimental.pallas import tpu as pltpu
from jax.sharding import PartitionSpec as P

F32, BF16 = jnp.float32, jnp.bfloat16
NAMES = ("w_gate", "w_up", "w_down")
BITS = (8, 4, 2)
VMEM_LIMIT = 66_000_000


def normed(h):
    wide = h.astype(F32)
    scale = lax.rsqrt(jnp.mean(wide**2, -1, keepdims=True) + 1e-6)
    return (wide * scale).astype(BF16)


def adamw(w, m, v, g):
    m = 0.9 * m + 0.1 * g
    v = 0.95 * v + 0.05 * g * g
    step = m * lax.rsqrt(v + 1e-8) + 0.1 * w
    return (w - 0.02 * step).astype(BF16), m, v


def clipped(gradients, sum_of_squares, count):
    factor = jnp.minimum(1.0, 0.5 * lax.rsqrt(sum_of_squares / count + 1e-30))
    return [g * factor for g in gradients]


def thirds(columns):
    tiles, start, out = columns // 128, 0, []
    for k in range(3):
        size = 128 * (tiles // 3 + (k < tiles % 3))
        out.append((start, size))
        start += size
    return out


class Place:
    def __init__(self):
        me = lax.axis_index("dp")
        self.core = me % 2
        self.at = (me // 8, (me // 4) % 2, (me // 2) % 2)
        self.near = tuple(me + bit * (1 - 2 * v) for bit, v in zip(BITS, self.at))
        self.twin = me + 1 - 2 * self.core

    def greet(self):
        barrier = pltpu.get_barrier_semaphore()
        for other in (*self.near, self.twin):
            pl.semaphore_signal(barrier, inc=1, device_id={"dp": other}, device_id_type=pl.DeviceIdType.MESH)
        pl.semaphore_wait(barrier, 4)


def remote(src, dst, send, recv, device):
    return pltpu.make_async_remote_copy(
        src_ref=src, dst_ref=dst, send_sem=send, recv_sem=recv, device_id={"dp": device}, device_id_type=pl.DeviceIdType.MESH
    )


class Gather:
    def __init__(self, place, own, full, send, recv, here):
        self.place, self.own, self.full, self.send, self.recv, self.here = place, own, full, send, recv, here
        self.cuts = thirds(own.shape[-1])

    def local(self):
        x, y, z = self.place.at
        return pltpu.make_async_copy(self.own, self.full.at[x, y, z, self.place.core], self.here)

    def copy(self, stage, k):
        order = [(k + j) % 3 for j in range(3)]
        at = list(self.place.at)
        for d in order[:stage]:
            at[d] = slice(None)
        columns = pl.ds(*self.cuts[k])
        region = self.full.at[(*at, self.place.core, slice(None), columns)]
        src = region if stage else self.own.at[:, columns]
        n = 3 * stage + k
        return remote(src, region, self.send.at[n], self.recv.at[n], self.place.near[order[stage]])

    def across(self):
        region = self.full.at[:, :, :, self.place.core]
        return remote(region, region, self.send.at[9], self.recv.at[9], self.place.twin)

    def act(self, j):
        if j == 0:
            self.local().start()
            for k in range(3):
                self.copy(0, k).start()
        elif j in (1, 2):
            if j == 1:
                self.local().wait()
            for k in range(3):
                self.copy(j - 1, k).wait_recv()
                self.copy(j, k).start()
        elif j == 3:
            for k in range(3):
                self.copy(2, k).wait_recv()
            self.across().start()
        else:
            self.across().wait_recv()
            for stage in range(3):
                for k in range(3):
                    self.copy(stage, k).wait_send()
            self.across().wait_send()


def gather_scratch():
    return [pltpu.SemaphoreType.DMA((10,)), pltpu.SemaphoreType.DMA((10,)), pltpu.SemaphoreType.DMA]


class Scatter:
    def __init__(self, place, partial, out, total, first, landed, send, recv, here):
        self.place, self.partial, self.out, self.total, self.first = place, partial, out, total, first
        self.landed, self.send, self.recv, self.here = landed, send, recv, here
        self.rows, self.columns = partial.shape[-2:]
        self.cuts = thirds(self.columns)
        self.strip = 16

    def load(self):
        return pltpu.make_async_copy(self.partial.at[:, :, :, self.place.core], self.total, self.here)

    def across(self):
        return remote(self.partial.at[:, :, :, 1 - self.place.core], self.first, self.send.at[9], self.recv.at[9], self.place.twin)

    def where(self, stage, k, keep):
        order = [(k + j) % 3 for j in range(3)]
        at = [slice(None)] * 3
        for d in order[:stage]:
            at[d] = self.place.at[d]
        d = order[stage]
        at[d] = self.place.at[d] if keep else 1 - self.place.at[d]
        return at, d

    def copy(self, stage, k):
        at, d = self.where(stage, k, False)
        n = 3 * stage + k
        return remote(
            self.total.at[(*at, slice(None), pl.ds(*self.cuts[k]))], self.landed[n], self.send.at[n], self.recv.at[n], self.place.near[d]
        )

    def add_first(self):
        @pl.loop(0, 8)
        def _(block):
            at = (block // 4, (block // 2) % 2, block % 2)

            @pl.loop(0, self.rows // self.strip)
            def _(strip):
                to = (*at, pl.ds(strip * self.strip, self.strip), slice(None))
                self.total[to] = (self.total[to].astype(F32) + self.first[to].astype(F32)).astype(BF16)

    def add(self, stage, k):
        at, _ = self.where(stage, k, True)
        landed, free = self.landed[3 * stage + k], [d for d in range(3) if isinstance(at[d], slice)]
        columns = pl.ds(*self.cuts[k])
        for number in range(2 ** len(free)):
            bits = [(number >> b) & 1 for b in reversed(range(len(free)))]
            spot = list(at)
            for d, bit in zip(free, bits):
                spot[d] = bit

            @pl.loop(0, self.rows // self.strip)
            def _(strip, spot=spot, bits=bits):
                rows = pl.ds(strip * self.strip, self.strip)
                to = (*spot, rows, columns)
                value = (self.total[to].astype(F32) + landed[(*bits, rows, slice(None))].astype(F32)).astype(BF16)
                if stage < 2:
                    self.total[to] = value
                else:
                    self.out[rows, columns] = value

    def act(self, j):
        if j == 0:
            self.across().start()
            self.load().start()
        elif j == 1:
            self.load().wait()
            self.across().wait_recv()
            self.add_first()
            for k in range(3):
                self.copy(0, k).start()
        elif j in (2, 3):
            for k in range(3):
                self.copy(j - 2, k).wait_recv()
                self.add(j - 2, k)
                self.copy(j - 1, k).start()
        else:
            for k in range(3):
                self.copy(2, k).wait_recv()
                self.add(2, k)
            for stage in range(3):
                for k in range(3):
                    self.copy(stage, k).wait_send()
            self.across().wait_send()


def scatter_scratch(rows, columns):
    landed = [pltpu.VMEM((2,) * (2 - stage) + (rows, size), BF16) for stage in range(3) for _, size in thirds(columns)]
    whole = pltpu.VMEM((2, 2, 2, rows, columns), BF16)
    return [whole, whole, *landed, pltpu.SemaphoreType.DMA((10,)), pltpu.SemaphoreType.DMA((10,)), pltpu.SemaphoreType.DMA]


ANY = pl.BlockSpec(memory_space=pl.ANY)


def once(shape):
    return pl.BlockSpec(shape, lambda i: (0,) * len(shape), pipeline_mode=pl.Buffered(1))


def fused(name, cid, steps, body, ins, in_specs, outs, out_specs, scratch, gathers=(), scatters=()):
    n_in, n_out = len(ins), len(outs)
    ng, ns = len(gathers), len(scatters)
    sizes = [w.shape[1:] for w, _, _ in gathers]
    in_specs, ins, outs, out_specs = list(in_specs), list(ins), list(outs), list(out_specs)
    scratch = list(scratch)
    n_scratch = len(scratch)
    for (w, layer, _), (r, c) in zip(gathers, sizes):
        ins.append(w)
        in_specs.append(pl.BlockSpec((1, r, c), lambda i, layer=layer: (layer, 0, 0), pipeline_mode=pl.Buffered(1)))
        outs.append(jax.ShapeDtypeStruct((2, 2, 2, 2, r, c), BF16))
        out_specs.append(ANY)
        scratch += gather_scratch()
    for d, _ in scatters:
        r, c = d.shape[-2:]
        ins.append(d)
        in_specs.append(ANY)
        outs.append(jax.ShapeDtypeStruct((r, c), BF16))
        out_specs.append(pl.BlockSpec((r, c), lambda i: (0, 0), pipeline_mode=pl.Buffered(1)))
        scratch += scatter_scratch(r, c)

    def kernel(*refs):
        refs = list(refs)
        i_refs, refs = refs[: n_in + ng + ns], refs[n_in + ng + ns :]
        o_refs, refs = refs[: n_out + ng + ns], refs[n_out + ng + ns :]
        own_scratch, refs = refs[:n_scratch], refs[n_scratch:]
        place = Place()
        exchanges = []
        for g in range(ng):
            exchanges.append((Gather(place, i_refs[n_in + g].at[0], o_refs[n_out + g], *refs[:3]), gathers[g][2]))
            refs = refs[3:]
        for s in range(ns):
            part, out = i_refs[n_in + ng + s], o_refs[n_out + ng + s]
            exchanges.append((Scatter(place, part, out, refs[0], refs[1], refs[2:11], *refs[11:14]), scatters[s][1]))
            refs = refs[14:]
        step = pl.program_id(0)

        def acts(at):
            for j in range(5):
                for exchange, when in exchanges:
                    if when[j] == at:
                        exchange.act(j)

        for at in sorted({w for _, when in exchanges for w in when if w < steps} | {0}):

            @pl.when(step == at)
            def _(at=at):
                if at == 0:
                    place.greet()
                acts(at)

        body(step, *i_refs[:n_in], *o_refs[:n_out], *own_scratch)

        @pl.when(step == steps - 1)
        def _():
            acts(steps)

    return pl.pallas_call(
        kernel,
        grid=(steps,),
        in_specs=in_specs,
        out_specs=out_specs,
        out_shape=outs,
        scratch_shapes=scratch,
        name=name,
        compiler_params=pltpu.CompilerParams(
            dimension_semantics=("arbitrary",), collective_id=cid, has_side_effects=True, vmem_limit_bytes=VMEM_LIMIT
        ),
    )(*ins)


def dot(a, b, contract=(1, 0)):
    return lax.dot_general(a, b, (((contract[0],), (contract[1],)), ((), ())), preferred_element_type=F32)


CHUNK = 512


def chunks(tokens, do):
    @pl.loop(0, tokens // CHUNK)
    def _(m):
        do(pl.ds(pl.multiple_of(m * CHUNK, CHUNK), CHUNK))


def forward_body(last, step, a, wg, wu, wd, gate, up, out, total):
    @pl.when(step == 0)
    def _():
        total[...] = jnp.zeros_like(total)

    def do(rows):
        g, u = dot(a[rows, :], wg[...]), dot(a[rows, :], wu[...])
        gate[rows, :], up[rows, :] = g, u
        hidden = (g * jax.nn.sigmoid(g) * u).astype(BF16)
        total[rows, :] += dot(hidden, wd[...])

    chunks(a.shape[0], do)

    @pl.when(step == last)
    def _():
        chunks(a.shape[0], lambda rows: out.__setitem__((rows, slice(None)), total[rows, :].astype(BF16)))


def forward_last_body(step, a, wg, wu, dy, gate, up, dwd, hidden):
    def do(rows):
        g, u = dot(a[rows, :], wg[...]), dot(a[rows, :], wu[...])
        gate[rows, :], up[rows, :] = g, u
        hidden[rows, :] = (g * jax.nn.sigmoid(g) * u).astype(BF16)

    chunks(a.shape[0], do)
    dwd[...] = dot(hidden[...], dy[...], (0, 0)).astype(BF16)


def through_gate(dy, wd, gate, up, dgate, dup, hidden, rows):
    by_hidden = dot(dy[rows, :], wd[...], (1, 1)).astype(BF16).astype(F32)
    g, u = gate[rows, :], up[rows, :]
    s = jax.nn.sigmoid(g)
    silu = g * s
    dup[rows, :] = (by_hidden * silu).astype(BF16)
    dgate[rows, :] = (by_hidden * u * (s + silu * (1.0 - s))).astype(BF16)
    if hidden is not None:
        hidden[rows, :] = (silu * u).astype(BF16)


def turn(a, at):
    for m in range(a.shape[0] // 256):
        at[:, m * 256 : (m + 1) * 256] = a[m * 256 : (m + 1) * 256, :].T


def back_last_body(step, dy, wd, gate, up, a, dgate, dup, dwg, dwu, at):
    @pl.when(step == 0)
    def _():
        turn(a, at)

    chunks(a.shape[0], lambda rows: through_gate(dy, wd, gate, up, dgate, dup, None, rows))
    dwg[...] = dot(at[...], dgate[...]).astype(BF16)
    dwu[...] = dot(at[...], dup[...]).astype(BF16)


def by_input_body(last, step, dgate, dup, wg, wu, out, total):
    @pl.when(step == 0)
    def _():
        total[...] = jnp.zeros_like(total)

    def do(rows):
        total[rows, :] += dot(dgate[rows, :], wg[...], (1, 1)) + dot(dup[rows, :], wu[...], (1, 1))

    chunks(dgate.shape[0], do)

    @pl.when(step == last)
    def _():
        chunks(dgate.shape[0], lambda rows: out.__setitem__((rows, slice(None)), total[rows, :].astype(BF16)))


def back_first_body(step, dy, wd, gate, up, dgate, dup, dwd, hidden):
    chunks(dy.shape[0], lambda rows: through_gate(dy, wd, gate, up, dgate, dup, hidden, rows))
    dwd[...] = dot(hidden[...], dy[...], (0, 0)).astype(BF16)


def weights_body(step, a, dgate, dup, dwg, dwu, at):
    @pl.when(step == 0)
    def _():
        turn(a, at)

    dwg[...] = dot(at[...], dgate[...]).astype(BF16)
    dwu[...] = dot(at[...], dup[...]).astype(BF16)


def nothing(step):
    pass


def solution(mesh):
    def step(x, dy, *arrays):
        weights, m, v = (arrays[i : i + 3] for i in (0, 3, 6))
        w_gate, w_up, w_down = weights
        x, dy = x[0], dy[0]
        tokens, d = x.shape
        ff = w_gate.shape[-1]
        tile = 256
        n = ff // tile

        def of(shape, dtype=BF16):
            return jax.ShapeDtypeStruct(shape, dtype)

        def columns(rows, width=tile):
            return pl.BlockSpec((rows, width), lambda i: (0, i))

        def rows_of(width, height=tile):
            return pl.BlockSpec((height, width), lambda i: (i, 0))

        def flat(full):
            return full.reshape(-1, full.shape[-1])

        def blocks(dw):
            return dw.reshape(2, 2, 2, 2, dw.shape[0] // 16, dw.shape[1])

        here = once((tokens, d))
        zero = (0,) * 5
        g0, u0, d0 = fused("fetch", 1, 1, nothing, [], [], [], [], [], gathers=[(w, 0, (0, 0, 0, 1, 1)) for w in weights])
        g0, u0, d0 = map(flat, (g0, u0, d0))
        a0 = normed(x)
        states = [of((tokens, ff), F32)] * 2
        gate0, up0, out0, g1, u1 = fused(
            "forward0", 2, n, functools.partial(forward_body, n - 1),
            [a0, g0, u0, d0], [here, columns(d), columns(d), rows_of(d)],
            [*states, of((tokens, d))], [columns(tokens), columns(tokens), here],
            [pltpu.VMEM((tokens, d), F32)],
            gathers=[(w_gate, 1, (0, 2, 5, 12, 15)), (w_up, 1, (0, 3, 7, n, n))],
        )
        g1, u1 = map(flat, (g1, u1))
        h1 = x + out0
        a1 = normed(h1)
        gate1, up1, dwd1, d1 = fused(
            "forward1", 3, n, forward_last_body,
            [a1, g1, u1, dy], [here, columns(d), columns(d), here],
            [*states, of((ff, d))], [columns(tokens), columns(tokens), rows_of(d)],
            [pltpu.VMEM((tokens, tile), BF16)],
            gathers=[(w_down, 1, (0, 2, 5, 10, 13))],
        )
        d1 = flat(d1)
        halves = [of((tokens, ff))] * 2
        dgate1, dup1, dwg1, dwu1, sd1 = fused(
            "back1", 4, n, back_last_body,
            [dy, d1, gate1, up1, a1], [here, rows_of(d), columns(tokens), columns(tokens), here],
            [*halves, of((d, ff)), of((d, ff))], [columns(tokens), columns(tokens), columns(d), columns(d)],
            [pltpu.VMEM((d, tokens), BF16)],
            scatters=[(blocks(dwd1), (0, 3, 8, 11, 13))],
        )
        wide = 512
        by_a1, sg1 = fused(
            "by_input1", 5, ff // wide, functools.partial(by_input_body, ff // wide - 1),
            [dgate1, dup1, g1, u1], [columns(tokens, wide), columns(tokens, wide), columns(d, wide), columns(d, wide)],
            [of((tokens, d))], [here],
            [pltpu.VMEM((tokens, d), F32)],
            scatters=[(blocks(dwg1), (0, 2, 6, 8, 8))],
        )
        (by_norm,) = jax.vjp(normed, h1)[1](by_a1)
        by_h = dy + by_norm
        dgate0, dup0, dwd0, su1 = fused(
            "back0", 6, n, back_first_body,
            [by_h, d0, gate0, up0], [here, rows_of(d), columns(tokens), columns(tokens)],
            [*halves, of((ff, d))], [columns(tokens), columns(tokens), rows_of(d)],
            [pltpu.VMEM((tokens, tile), BF16)],
            scatters=[(blocks(dwu1), (0, 4, 11, 15, n))],
        )
        dwg0, dwu0, sd0 = fused(
            "weights0", 7, n, weights_body,
            [a0, dgate0, dup0], [here, columns(tokens), columns(tokens)],
            [of((d, ff)), of((d, ff))], [columns(d), columns(d)],
            [pltpu.VMEM((d, tokens), BF16)],
            scatters=[(blocks(dwd0), (0, 4, 11, 15, n))],
        )
        sg0, su0 = fused("finish", 8, 1, nothing, [], [], [], [], [], scatters=[(blocks(dw), (0, 0, 1, 1, 1)) for dw in (dwg0, dwu0)])
        gradients = [jnp.stack(pair).astype(F32) for pair in ((sg0, sg1), (su0, su1), (sd0, sd1))]
        squares = lax.psum(sum(jnp.sum(g * g) for g in gradients), "dp")
        gradients = clipped(gradients, squares, lax.psum(1, "dp") * sum(g.size for g in gradients))
        new = [adamw(w.astype(F32), m, v, g) for w, m, v, g in zip(weights, m, v, gradients, strict=True)]
        return tuple(one[which] for which in range(3) for one in new)

    states, cut = P(("rep", "dp"), None, None), P(None, "dp", None)
    return jax.shard_map(
        step,
        mesh=mesh,
        in_specs=(states, states) + (cut,) * 9,
        out_specs=(P("rep", "dp", None),) * 9,
        check_vma=False,
    )
```

```python
import functools

import jax
import jax.numpy as jnp
from jax import lax
from jax.experimental import pallas as pl
from jax.experimental.pallas import tpu as pltpu
from jax.sharding import PartitionSpec as P

F32, BF16 = jnp.float32, jnp.bfloat16
NAMES = ("w_gate", "w_up", "w_down")
BITS = (8, 4, 2)
DEVICES = 16
VMEM_LIMIT = 67_000_000


def adamw(w, m, v, g):
    m = 0.9 * m + 0.1 * g
    v = 0.95 * v + 0.05 * g * g
    step = m * lax.rsqrt(v + 1e-8) + 0.1 * w
    return (w - 0.02 * step).astype(BF16), m, v


def clipped(gradients, sum_of_squares, count):
    factor = jnp.minimum(1.0, 0.5 * lax.rsqrt(sum_of_squares / count + 1e-30))
    return [g * factor for g in gradients]


def thirds(columns):
    tiles, start, out = columns // 128, 0, []
    for k in range(3):
        size = 128 * (tiles // 3 + (k < tiles % 3))
        out.append((start, size))
        start += size
    return out


class Place:
    def __init__(self):
        me = self.me = lax.axis_index("dp")
        self.core = me % 2
        self.at = (me // 8, (me // 4) % 2, (me // 2) % 2)
        self.near = tuple(me + bit * (1 - 2 * v) for bit, v in zip(BITS, self.at))
        self.twin = me + 1 - 2 * self.core

    def greet(self, everyone):
        barrier = pltpu.get_barrier_semaphore()
        others = [(self.me + k) % DEVICES for k in range(1, DEVICES)] if everyone else [*self.near, self.twin]
        for other in others:
            pl.semaphore_signal(barrier, inc=1, device_id={"dp": other}, device_id_type=pl.DeviceIdType.MESH)
        pl.semaphore_wait(barrier, len(others))


def remote(src, dst, send, recv, device):
    return pltpu.make_async_remote_copy(
        src_ref=src, dst_ref=dst, send_sem=send, recv_sem=recv, device_id={"dp": device}, device_id_type=pl.DeviceIdType.MESH
    )


class Gather:
    def __init__(self, place, own, full, send, recv, here):
        self.place, self.own, self.full, self.send, self.recv, self.here = place, own, full, send, recv, here
        self.cuts = thirds(own.shape[-1])

    def local(self):
        x, y, z = self.place.at
        return pltpu.make_async_copy(self.own, self.full.at[x, y, z, self.place.core], self.here)

    def copy(self, stage, k):
        order = [(k + j) % 3 for j in range(3)]
        at = list(self.place.at)
        for d in order[:stage]:
            at[d] = slice(None)
        columns = pl.ds(*self.cuts[k])
        region = self.full.at[(*at, self.place.core, slice(None), columns)]
        src = region if stage else self.own.at[:, columns]
        n = 3 * stage + k
        return remote(src, region, self.send.at[n], self.recv.at[n], self.place.near[order[stage]])

    def across(self):
        region = self.full.at[:, :, :, self.place.core]
        return remote(region, region, self.send.at[9], self.recv.at[9], self.place.twin)

    def act(self, j):
        if j == 0:
            self.local().start()
            for k in range(3):
                self.copy(0, k).start()
        elif j in (1, 2):
            if j == 1:
                self.local().wait()
            for k in range(3):
                self.copy(j - 1, k).wait_recv()
                self.copy(j, k).start()
        elif j == 3:
            for k in range(3):
                self.copy(2, k).wait_recv()
            self.across().start()
        else:
            self.across().wait_recv()
            for stage in range(3):
                for k in range(3):
                    self.copy(stage, k).wait_send()
            self.across().wait_send()


class Scatter:
    def __init__(self, place, partial, out, total, first, landed, send, recv, here):
        self.place, self.partial, self.out, self.total, self.first = place, partial, out, total, first
        self.landed, self.send, self.recv, self.here = landed, send, recv, here
        self.rows, self.columns = partial.shape[-2:]
        self.cuts = thirds(self.columns)
        self.strip = 16
        self.kept = total is None
        self.sums, self.half = (partial, (place.core,)) if self.kept else (total, ())

    def load(self):
        return pltpu.make_async_copy(self.partial.at[:, :, :, self.place.core], self.total, self.here)

    def across(self):
        return remote(self.partial.at[:, :, :, 1 - self.place.core], self.first, self.send.at[9], self.recv.at[9], self.place.twin)

    def where(self, stage, k, keep):
        order = [(k + j) % 3 for j in range(3)]
        at = [slice(None)] * 3
        for d in order[:stage]:
            at[d] = self.place.at[d]
        d = order[stage]
        at[d] = self.place.at[d] if keep else 1 - self.place.at[d]
        return at, d

    def copy(self, stage, k):
        at, d = self.where(stage, k, False)
        n = 3 * stage + k
        src = self.sums.at[(*at, *self.half, slice(None), pl.ds(*self.cuts[k]))]
        return remote(src, self.landed[n], self.send.at[n], self.recv.at[n], self.place.near[d])

    def add_first(self):
        @pl.loop(0, 8)
        def _(block):
            at = (block // 4, (block // 2) % 2, block % 2)

            @pl.loop(0, self.rows // self.strip)
            def _(strip):
                rest = (pl.ds(strip * self.strip, self.strip), slice(None))
                to = (*at, *self.half, *rest)
                self.sums[to] = (self.sums[to].astype(F32) + self.first[(*at, *rest)].astype(F32)).astype(BF16)

    def add(self, stage, k):
        at, _ = self.where(stage, k, True)
        landed, free = self.landed[3 * stage + k], [d for d in range(3) if isinstance(at[d], slice)]
        columns = pl.ds(*self.cuts[k])
        for number in range(2 ** len(free)):
            bits = [(number >> b) & 1 for b in reversed(range(len(free)))]
            spot = list(at)
            for d, bit in zip(free, bits):
                spot[d] = bit

            @pl.loop(0, self.rows // self.strip)
            def _(strip, spot=spot, bits=bits):
                rows = pl.ds(strip * self.strip, self.strip)
                to = (*spot, *self.half, rows, columns)
                value = (self.sums[to].astype(F32) + landed[(*bits, rows, slice(None))].astype(F32)).astype(BF16)
                if stage < 2:
                    self.sums[to] = value
                else:
                    self.out[rows, columns] = value

    def act(self, j):
        if j == 0:
            self.across().start()
            if not self.kept:
                self.load().start()
        elif j == 1:
            if not self.kept:
                self.load().wait()
            self.across().wait_recv()
            self.add_first()
            for k in range(3):
                self.copy(0, k).start()
        elif j in (2, 3):
            for k in range(3):
                self.copy(j - 2, k).wait_recv()
                self.add(j - 2, k)
                self.copy(j - 1, k).start()
        else:
            for k in range(3):
                self.copy(2, k).wait_recv()
                self.add(2, k)
            for stage in range(3):
                for k in range(3):
                    self.copy(stage, k).wait_send()
            self.across().wait_send()


def scatter_scratch(rows, columns, kept=False):
    landed = [pltpu.VMEM((2,) * (2 - stage) + (rows, size), BF16) for stage in range(3) for _, size in thirds(columns)]
    half = pltpu.VMEM((2, 2, 2, rows, columns), BF16)
    mine = pltpu.VMEM((2, 2, 2, 2, rows, columns), BF16) if kept else half
    return [mine, half, *landed, pltpu.SemaphoreType.DMA((10,)), pltpu.SemaphoreType.DMA((10,)), pltpu.SemaphoreType.DMA]


class Norm:
    def __init__(self, place, own, all_of, out, send, recv):
        self.place, self.own, self.all_of, self.out, self.send, self.recv = place, own, all_of, out, send, recv

    def exchange(self):
        me, others = self.place.me, [(self.place.me + k) % DEVICES for k in range(1, DEVICES)]
        copies = [remote(self.own, self.all_of.at[me], self.send.at[k], self.recv.at[me], other) for k, other in enumerate(others)]
        for copy in copies:
            copy.start()
        self.all_of[me] = self.own[...]
        for k, other in enumerate(others):
            remote(self.own, self.all_of.at[other], self.send.at[k], self.recv.at[other], other).wait_recv()
        for copy in copies:
            copy.wait_send()
        total = self.all_of[0]
        for k in range(1, DEVICES):
            total = total + self.all_of[k]
        self.out[...] = total


ANY = pl.BlockSpec(memory_space=pl.ANY)


def once(shape):
    return pl.BlockSpec(shape, lambda i: (0,) * len(shape), pipeline_mode=pl.Buffered(1))


def fused(name, cid, steps, body, ins, in_specs, outs, out_specs, scratch, gathers=(), scatters=(), kept=(), norm_of=(), see=False, prelude=None):
    n_in, n_out = len(ins), len(outs)
    ng, ns, nk, nn = len(gathers), len(scatters), len(kept), len(norm_of)
    in_specs, ins, outs, out_specs = list(in_specs), list(ins), list(outs), list(out_specs)
    scratch = list(scratch)
    n_scratch = len(scratch)
    for w, layer, _ in gathers:
        r, c = w.shape[1:]
        ins.append(w)
        in_specs.append(pl.BlockSpec((1, r, c), lambda i, layer=layer: (layer, 0, 0), pipeline_mode=pl.Buffered(1)))
        outs.append(jax.ShapeDtypeStruct((2, 2, 2, 2, r, c), BF16))
        out_specs.append(ANY)
        scratch += [pltpu.SemaphoreType.DMA((10,)), pltpu.SemaphoreType.DMA((10,)), pltpu.SemaphoreType.DMA]
    for d, _ in scatters:
        ins.append(d)
        in_specs.append(ANY)
    for r, c in [d.shape[-2:] for d, _ in scatters] + [k[:2] for k in kept]:
        outs.append(jax.ShapeDtypeStruct((r, c), BF16))
        out_specs.append(pl.BlockSpec((r, c), lambda i: (0, 0), pipeline_mode=pl.Buffered(1)))
    for d, _ in scatters:
        scratch += scatter_scratch(*d.shape[-2:])
    for r, c, _ in kept:
        scratch += scatter_scratch(r, c, True)
    for g in norm_of:
        ins.append(g)
        in_specs.append(once(g.shape))
    if nn:
        outs.append(jax.ShapeDtypeStruct((8, 128), F32))
        out_specs.append(once((8, 128)))
        scratch += [pltpu.VMEM((8, 128), F32), pltpu.VMEM((DEVICES, 8, 128), F32)]
        scratch += [pltpu.SemaphoreType.DMA((DEVICES,)), pltpu.SemaphoreType.DMA((DEVICES,))]

    def kernel(*refs):
        refs = list(refs)

        def take(n):
            taken, refs[:n] = refs[:n], []
            return taken

        body_in, own, partial, known = take(n_in), take(ng), take(ns), take(nn)
        body_out, full, mine, sum_out = take(n_out), take(ng), take(ns + nk), take(1 if nn else 0)
        own_scratch = take(n_scratch)
        place = Place()
        exchanges = [(Gather(place, own[g].at[0], full[g], *take(3)), gathers[g][2]) for g in range(ng)]
        for s in range(ns):
            got = take(14)
            exchanges.append((Scatter(place, partial[s], mine[s], got[0], got[1], got[2:11], *got[11:]), scatters[s][1]))
        for k in range(nk):
            got = take(14)
            own_scratch.append(got[0])
            exchanges.append((Scatter(place, got[0], mine[ns + k], None, got[1], got[2:11], *got[11:]), kept[k][2]))
        step = pl.program_id(0)
        acts = sorted([(at, n, j) for n, (_, when) in enumerate(exchanges) for j, at in enumerate(when)] + [(0.05, -1, 0)] * bool(prelude))

        def due(place_of):
            for at, n, j in acts:
                if int(at) == place_of:
                    if n < 0:
                        prelude(*body_in, *body_out)
                    else:
                        exchanges[n][0].act(j)

        for at in sorted({int(at) for at, _, _ in acts if at < steps} | {0}):

            @pl.when(step == at)
            def _(at=at):
                if at == 0:
                    place.greet(bool(nn))
                due(at)

        body(step, *body_in, *body_out, *own_scratch, *(full if see else ()))

        @pl.when(step == steps - 1)
        def _():
            due(steps)
            if nn:
                one = sum(squares(ref) for ref in (*known, *mine))
                norm = Norm(place, *take(1), *take(1), sum_out[0], *take(2))
                norm.own[...] = jnp.full((8, 128), one, F32)
                norm.exchange()

    return pl.pallas_call(
        kernel,
        grid=(steps,),
        in_specs=in_specs,
        out_specs=out_specs,
        out_shape=outs,
        scratch_shapes=scratch,
        name=name,
        compiler_params=pltpu.CompilerParams(
            dimension_semantics=("arbitrary",), collective_id=cid, has_side_effects=True, vmem_limit_bytes=VMEM_LIMIT
        ),
    )(*ins)


def squares(ref):
    rows, columns = ref.shape

    def strip(s, total):
        part = ref[pl.ds(s * 16, 16), :].astype(F32)
        part = part * part
        return total + sum(part[:, c : c + 128] for c in range(0, columns, 128))

    return jnp.sum(lax.fori_loop(0, rows // 16, strip, jnp.zeros((16, 128), F32)))


def dot(a, b, contract=(1, 0)):
    return lax.dot_general(a, b, (((contract[0],), (contract[1],)), ((), ())), preferred_element_type=F32)


CHUNK = 512


def chunks(tokens, do, unroll=True):
    @pl.loop(0, tokens // CHUNK, unroll=unroll)
    def _(m):
        do(pl.ds(pl.multiple_of(m * CHUNK, CHUNK), CHUNK))


def strips(tokens, do):
    @pl.loop(0, tokens // 64)
    def _(m):
        do(pl.ds(pl.multiple_of(m * 64, 64), 64))


def normed(h):
    wide = h.astype(F32)
    return (wide * lax.rsqrt(jnp.mean(wide**2, -1, keepdims=True) + 1e-6)).astype(BF16)


def normed_back(h, by_a):
    wide, by_a = h.astype(F32), by_a.astype(F32)
    scale = lax.rsqrt(jnp.mean(wide**2, -1, keepdims=True) + 1e-6)
    return (by_a * scale - wide * (scale * scale * scale * jnp.mean(by_a * wide, -1, keepdims=True))).astype(BF16)


def forward_prelude(x, a, *_):
    def do(rows):
        a[rows, :] = normed(x[rows, :])

    strips(x.shape[0], do)


def forward_body(tiles, step, x, a, gate, up, h, a_next, hidden, w, wd, w_sem, wd_sem, g_full, u_full, d_full, *_):
    width = gate.shape[1]

    def copy(t, slot, m):
        columns = pl.ds(pl.multiple_of(t * width, width), width)
        return pltpu.make_async_copy((g_full, u_full)[m].at[:, :, :, :, :, columns], w.at[slot, m], w_sem.at[slot, m])

    @pl.when((step >= 1) & (step <= tiles))
    def _():
        t = step - 1
        slot = t % 2

        @pl.when(t == 0)
        def _():
            for m in range(2):
                copy(t, slot, m).start()

        @pl.when(t + 1 < tiles)
        def _():
            for m in range(2):
                copy(t + 1, 1 - slot, m).start()

        for m in range(2):
            copy(t, slot, m).wait()
        columns = pl.ds(pl.multiple_of(t * width, width), width)

        def do(rows):
            g = dot(a[rows, :], w[slot, 0].reshape(-1, width))
            u = dot(a[rows, :], w[slot, 1].reshape(-1, width))
            gate[rows, :], up[rows, :] = g, u
            hidden[rows, columns] = (g * jax.nn.sigmoid(g) * u).astype(BF16)

        chunks(a.shape[0], do)

    @pl.when(step == tiles + 1)
    def _():
        pltpu.make_async_copy(d_full, wd, wd_sem).start()
        pltpu.make_async_copy(d_full, wd, wd_sem).wait()

    @pl.when(step > tiles)
    def _():
        height = h.shape[0]
        rows = pl.ds(pl.multiple_of((step - tiles - 1) * height, height), height)
        out = dot(hidden[rows, :], wd[...].reshape(-1, wd.shape[-1])).astype(BF16).astype(F32)
        new = (x[rows, :].astype(F32) + out).astype(BF16)
        h[...] = new
        a_next[...] = normed(new)


def forward_last_body(step, a, wg, wu, dy, gate, up, dwd, hidden):
    def do(rows):
        g, u = dot(a[rows, :], wg[...]), dot(a[rows, :], wu[...])
        gate[rows, :], up[rows, :] = g, u
        hidden[rows, :] = (g * jax.nn.sigmoid(g) * u).astype(BF16)

    chunks(a.shape[0], do)
    dwd[...] = dot(hidden[...], dy[...], (0, 0)).astype(BF16)


def through_gate(dy, wd, gate, up, dgate, dup, hidden, rows):
    by_hidden = dot(dy[rows, :], wd[...], (1, 1)).astype(BF16).astype(F32)
    g, u = gate[rows, :], up[rows, :]
    s = jax.nn.sigmoid(g)
    silu = g * s
    dup[rows, :] = (by_hidden * silu).astype(BF16)
    dgate[rows, :] = (by_hidden * u * (s + silu * (1.0 - s))).astype(BF16)
    if hidden is not None:
        hidden[rows, :] = (silu * u).astype(BF16)


def turn(a, at):
    for m in range(a.shape[0] // 256):
        at[:, m * 256 : (m + 1) * 256] = a[m * 256 : (m + 1) * 256, :].T


def back_last_body(step, dy, wd, gate, up, a, dgate, dup, dwg, at):
    @pl.when(step == 0)
    def _():
        turn(a, at)

    chunks(a.shape[0], lambda rows: through_gate(dy, wd, gate, up, dgate, dup, None, rows))
    dwg[...] = dot(at[...], dgate[...]).astype(BF16)


def by_input_body(last, step, dgate, dup, wg, wu, h, dy, at, by_h, dwu, total):
    @pl.when(step == 0)
    def _():
        total[...] = jnp.zeros_like(total)

    def do(rows):
        total[rows, :] += dot(dgate[rows, :], wg[...], (1, 1)) + dot(dup[rows, :], wu[...], (1, 1))

    chunks(dgate.shape[0], do)
    dwu[...] = dot(at[...], dup[...]).astype(BF16)

    @pl.when(step == last)
    def _():
        def finish(rows):
            by_norm = normed_back(h[rows, :], total[rows, :].astype(BF16))
            by_h[rows, :] = (dy[rows, :].astype(F32) + by_norm.astype(F32)).astype(BF16)

        strips(dgate.shape[0], finish)


def back_first_body(step, dy, wd, gate, up, dgate, dup, dwd, hidden):
    chunks(dy.shape[0], lambda rows: through_gate(dy, wd, gate, up, dgate, dup, hidden, rows))
    dwd[...] = dot(hidden[...], dy[...], (0, 0)).astype(BF16)


def weights_body(half, step, a, dgate, dup, at, dwg, dwu):
    @pl.when(step == 0)
    def _():
        turn(a, at)

    for number, (d, dw) in enumerate(((dgate, dwg), (dup, dwu))):

        @pl.when(step // half == number)
        def _(d=d, dw=dw, number=number):
            width = d.shape[1]
            columns = pl.ds(pl.multiple_of((step - number * half) * width, width), width)
            dw[:, :, :, :, :, columns] = dot(at[...], d[...]).astype(BF16).reshape(*dw.shape[:5], width)


def solution(mesh):
    def step(x, dy, *arrays):
        weights, m, v = (arrays[i : i + 3] for i in (0, 3, 6))
        w_gate, w_up, w_down = weights
        x, dy = x[0], dy[0]
        tokens, d = x.shape
        ff = w_gate.shape[-1]
        tile = 256
        n = ff // tile

        def of(shape, dtype=BF16):
            return jax.ShapeDtypeStruct(shape, dtype)

        def columns(rows, width=tile):
            return pl.BlockSpec((rows, width), lambda i: (0, i))

        def rows_of(width, height=tile):
            return pl.BlockSpec((height, width), lambda i: (i, 0))

        def flat(full):
            return full.reshape(-1, full.shape[-1])

        def blocks(dw):
            return dw.reshape(2, 2, 2, 2, dw.shape[0] // 16, dw.shape[1])

        here = once((tokens, d))
        states = [of((tokens, ff), F32)] * 2
        halves = [of((tokens, ff))] * 2
        height = 256
        parts = tokens // height
        last = 1 + n + parts

        def tiles_of(i):
            return (0, jnp.clip(i - 1, 0, n - 1))

        def parts_of(i):
            return (jnp.clip(i - 1 - n, 0, parts - 1), 0)

        a0, gate0, up0, h1, a1, _, _, d0, g1, u1 = fused(
            "forward0", 2, last, functools.partial(forward_body, n), [x], [here],
            [of((tokens, d)), *states, of((tokens, d)), of((tokens, d))],
            [here, *[pl.BlockSpec((tokens, tile), tiles_of)] * 2, *[pl.BlockSpec((height, d), parts_of)] * 2],
            [
                pltpu.VMEM((tokens, ff), BF16), pltpu.VMEM((2, 2, 2, 2, 2, 2, d // DEVICES, tile), BF16),
                pltpu.VMEM((2, 2, 2, 2, ff // DEVICES, d), BF16), pltpu.SemaphoreType.DMA((2, 2)), pltpu.SemaphoreType.DMA,
            ],
            gathers=[
                (w_gate, 0, (0, 0.10, 0.20, 0.30, 0.50)),
                (w_up, 0, (0, 0.11, 0.21, 0.40, 0.51)),
                (w_down, 0, (0.22, 0.60, 6, 14, n + 1)),
                (w_gate, 1, (0.23, 0.61, 12, n + 7, last + 0.4)),
                (w_up, 1, (0.24, 6.5, n + 1.5, last + 0.1, last + 0.5)),
            ],
            see=True, prelude=forward_prelude,
        )
        d0 = flat(d0)
        g1, u1 = map(flat, (g1, u1))
        gate1, up1, dwd1, d1 = fused(
            "forward1", 3, n, forward_last_body,
            [a1, g1, u1, dy], [here, columns(d), columns(d), here],
            [*states, of((ff, d))], [columns(tokens), columns(tokens), rows_of(d)],
            [pltpu.VMEM((tokens, tile), BF16)],
            gathers=[(w_down, 1, (0, 2, 5, 10, 14))],
        )
        d1 = flat(d1)
        dgate1, dup1, dwg1, a1_t, sd1 = fused(
            "back1", 4, n, back_last_body,
            [dy, d1, gate1, up1, a1], [here, rows_of(d), columns(tokens), columns(tokens), here],
            [*halves, of((d, ff)), of((d, tokens))], [columns(tokens), columns(tokens), columns(d), once((d, tokens))],
            [],
            scatters=[(blocks(dwd1), (0, 3, 9, 12, 15))],
        )
        by_h, dwu1, sg1 = fused(
            "by_input1", 5, n, functools.partial(by_input_body, n - 1),
            [dgate1, dup1, g1, u1, h1, dy, a1_t],
            [columns(tokens), columns(tokens), columns(d), columns(d), here, here, once((d, tokens))],
            [of((tokens, d)), of((d, ff))], [here, columns(d)],
            [pltpu.VMEM((tokens, d), F32)],
            scatters=[(blocks(dwg1), (0, 3, 8, 11, 13))],
        )
        dgate0, dup0, dwd0, su1 = fused(
            "back0", 6, n, back_first_body,
            [by_h, d0, gate0, up0], [here, rows_of(d), columns(tokens), columns(tokens)],
            [*halves, of((ff, d))], [columns(tokens), columns(tokens), rows_of(d)],
            [pltpu.VMEM((tokens, tile), BF16)],
            scatters=[(blocks(dwu1), (0, 3, 9, 12, 15))],
        )
        sd0, sg0, su0, squares_sum = fused(
            "finish", 7, 2 * n, functools.partial(weights_body, n),
            [a0, dgate0, dup0],
            [
                here,
                pl.BlockSpec((tokens, tile), lambda i: (0, jnp.minimum(i, n - 1))),
                pl.BlockSpec((tokens, tile), lambda i: (0, jnp.maximum(i - n, 0))),
            ],
            [], [], [pltpu.VMEM((d, tokens), BF16)],
            scatters=[(blocks(dwd0), (0, 8, 22, 30, 2 * n + 0.1))],
            kept=[
                (d // 16, ff, (n, 25, 2 * n + 0.2, 2 * n + 0.4, 2 * n + 0.6)),
                (d // 16, ff, (2 * n, 2 * n + 0.05, 2 * n + 0.5, 2 * n + 0.7, 2 * n + 0.8)),
            ],
            norm_of=[sg1, su1, sd1],
        )
        gradients = [jnp.stack(pair).astype(F32) for pair in ((sg0, sg1), (su0, su1), (sd0, sd1))]
        gradients = clipped(gradients, squares_sum[0, 0], DEVICES * sum(g.size for g in gradients))
        new = [adamw(w.astype(F32), m, v, g) for w, m, v, g in zip(weights, m, v, gradients, strict=True)]
        return tuple(one[which] for which in range(3) for one in new)

    states, cut = P(("rep", "dp"), None, None), P(None, "dp", None)
    return jax.shard_map(
        step,
        mesh=mesh,
        in_specs=(states, states) + (cut,) * 9,
        out_specs=(P("rep", "dp", None),) * 9,
        check_vma=False,
    )
```

```python
import functools

import jax
import jax.numpy as jnp
from jax import lax
from jax.experimental import pallas as pl
from jax.experimental.pallas import tpu as pltpu
from jax.sharding import PartitionSpec as P

F32, BF16 = jnp.float32, jnp.bfloat16
NAMES = ("w_gate", "w_up", "w_down")
BITS = (8, 4, 2)
DEVICES = 16
VMEM_LIMIT = 67_000_000


def adamw(w, m, v, g):
    m = 0.9 * m + 0.1 * g
    v = 0.95 * v + 0.05 * g * g
    step = m * lax.rsqrt(v + 1e-8) + 0.1 * w
    return (w - 0.02 * step).astype(BF16), m, v


def clipped(gradients, sum_of_squares, count):
    factor = jnp.minimum(1.0, 0.5 * lax.rsqrt(sum_of_squares / count + 1e-30))
    return [g * factor for g in gradients]


def thirds(columns):
    tiles, start, out = columns // 128, 0, []
    for k in range(3):
        size = 128 * (tiles // 3 + (k < tiles % 3))
        out.append((start, size))
        start += size
    return out


class Place:
    def __init__(self):
        me = self.me = lax.axis_index("dp")
        self.core = me % 2
        self.at = (me // 8, (me // 4) % 2, (me // 2) % 2)
        self.near = tuple(me + bit * (1 - 2 * v) for bit, v in zip(BITS, self.at))
        self.twin = me + 1 - 2 * self.core

    def greet(self, everyone):
        barrier = pltpu.get_barrier_semaphore()
        others = [(self.me + k) % DEVICES for k in range(1, DEVICES)] if everyone else [*self.near, self.twin]
        for other in others:
            pl.semaphore_signal(barrier, inc=1, device_id={"dp": other}, device_id_type=pl.DeviceIdType.MESH)
        pl.semaphore_wait(barrier, len(others))


def remote(src, dst, send, recv, device):
    return pltpu.make_async_remote_copy(
        src_ref=src, dst_ref=dst, send_sem=send, recv_sem=recv, device_id={"dp": device}, device_id_type=pl.DeviceIdType.MESH
    )


class Gather:
    def __init__(self, place, own, full, send, recv, here):
        self.place, self.own, self.full, self.send, self.recv, self.here = place, own, full, send, recv, here
        self.cuts = thirds(own.shape[-1])

    def local(self):
        x, y, z = self.place.at
        return pltpu.make_async_copy(self.own, self.full.at[x, y, z, self.place.core], self.here)

    def copy(self, stage, k):
        order = [(k + j) % 3 for j in range(3)]
        at = list(self.place.at)
        for d in order[:stage]:
            at[d] = slice(None)
        columns = pl.ds(*self.cuts[k])
        region = self.full.at[(*at, self.place.core, slice(None), columns)]
        src = region if stage else self.own.at[:, columns]
        n = 3 * stage + k
        return remote(src, region, self.send.at[n], self.recv.at[n], self.place.near[order[stage]])

    def across(self):
        region = self.full.at[:, :, :, self.place.core]
        return remote(region, region, self.send.at[9], self.recv.at[9], self.place.twin)

    def act(self, j):
        if j == 0:
            self.local().start()
            for k in range(3):
                self.copy(0, k).start()
        elif j in (1, 2):
            if j == 1:
                self.local().wait()
            for k in range(3):
                self.copy(j - 1, k).wait_recv()
                self.copy(j, k).start()
        elif j == 3:
            for k in range(3):
                self.copy(2, k).wait_recv()
            self.across().start()
        else:
            self.across().wait_recv()
            for stage in range(3):
                for k in range(3):
                    self.copy(stage, k).wait_send()
            self.across().wait_send()


class Scatter:
    def __init__(self, place, partial, out, total, first, landed, send, recv, here):
        self.place, self.partial, self.out, self.total, self.first = place, partial, out, total, first
        self.landed, self.send, self.recv, self.here = landed, send, recv, here
        self.rows, self.columns = partial.shape[-2:]
        self.cuts = thirds(self.columns)
        self.strip = 16
        self.kept, self.paired = total is None, len(partial.shape) == 5
        self.sums, self.half = (partial, (place.core,)) if self.kept else (total, ())

    def load(self):
        mine = self.partial if self.paired else self.partial.at[:, :, :, self.place.core]
        return pltpu.make_async_copy(mine, self.total, self.here)

    def across(self):
        return remote(self.partial.at[:, :, :, 1 - self.place.core], self.first, self.send.at[9], self.recv.at[9], self.place.twin)

    def where(self, stage, k, keep):
        order = [(k + j) % 3 for j in range(3)]
        at = [slice(None)] * 3
        for d in order[:stage]:
            at[d] = self.place.at[d]
        d = order[stage]
        at[d] = self.place.at[d] if keep else 1 - self.place.at[d]
        return at, d

    def copy(self, stage, k):
        at, d = self.where(stage, k, False)
        n = 3 * stage + k
        src = self.sums.at[(*at, *self.half, slice(None), pl.ds(*self.cuts[k]))]
        return remote(src, self.landed[n], self.send.at[n], self.recv.at[n], self.place.near[d])

    def add_first(self):
        @pl.loop(0, 8)
        def _(block):
            at = (block // 4, (block // 2) % 2, block % 2)

            @pl.loop(0, self.rows // self.strip)
            def _(strip):
                rest = (pl.ds(strip * self.strip, self.strip), slice(None))
                to = (*at, *self.half, *rest)
                self.sums[to] = (self.sums[to].astype(F32) + self.first[(*at, *rest)].astype(F32)).astype(BF16)

    def add(self, stage, k):
        at, _ = self.where(stage, k, True)
        landed, free = self.landed[3 * stage + k], [d for d in range(3) if isinstance(at[d], slice)]
        columns = pl.ds(*self.cuts[k])
        for number in range(2 ** len(free)):
            bits = [(number >> b) & 1 for b in reversed(range(len(free)))]
            spot = list(at)
            for d, bit in zip(free, bits):
                spot[d] = bit

            @pl.loop(0, self.rows // self.strip)
            def _(strip, spot=spot, bits=bits):
                rows = pl.ds(strip * self.strip, self.strip)
                to = (*spot, *self.half, rows, columns)
                value = (self.sums[to].astype(F32) + landed[(*bits, rows, slice(None))].astype(F32)).astype(BF16)
                if stage < 2:
                    self.sums[to] = value
                else:
                    self.out[rows, columns] = value

    def act(self, j):
        if j == 0:
            if not self.paired:
                self.across().start()
            if not self.kept:
                self.load().start()
        elif j == 1:
            if not self.kept:
                self.load().wait()
            if not self.paired:
                self.across().wait_recv()
                self.add_first()
            for k in range(3):
                self.copy(0, k).start()
        elif j in (2, 3):
            for k in range(3):
                self.copy(j - 2, k).wait_recv()
                self.add(j - 2, k)
                self.copy(j - 1, k).start()
        else:
            for k in range(3):
                self.copy(2, k).wait_recv()
                self.add(2, k)
            for stage in range(3):
                for k in range(3):
                    self.copy(stage, k).wait_send()
            if not self.paired:
                self.across().wait_send()


def scatter_scratch(rows, columns, kept=False, paired=False):
    landed = [pltpu.VMEM((2,) * (2 - stage) + (rows, size), BF16) for stage in range(3) for _, size in thirds(columns)]
    half = pltpu.VMEM((2, 2, 2, rows, columns), BF16)
    mine = pltpu.VMEM((2, 2, 2, 2, rows, columns), BF16) if kept else half
    return [mine, pltpu.VMEM((8, 128), BF16) if paired else half, *landed, pltpu.SemaphoreType.DMA((10,)), pltpu.SemaphoreType.DMA((10,)), pltpu.SemaphoreType.DMA]


class Pair:
    def __init__(self, place, steps, out, partial, landed, send, recv):
        self.place, self.out, self.partial, self.landed, self.send, self.recv = place, out, partial, landed, send, recv
        self.rows, self.columns = partial.shape[-2:]
        self.steps, self.whole = steps, steps == DEVICES and self.rows * DEVICES > self.columns

    def copy(self, number):
        if self.whole:
            block = (number // 8, (number // 4) % 2, (number // 2) % 2)
            src, dst = self.partial.at[(*block, number % 2)], self.landed.at[block]
        else:
            width = self.columns // self.steps
            columns = pl.ds(pl.multiple_of(number * width, width), width)
            src = self.partial.at[:, :, :, 1 - self.place.core, :, columns]
            dst = self.landed.at[:, :, :, :, columns]
        return remote(src, dst, self.send.at[number], self.recv.at[number], self.place.twin)

    def made(self, number):
        if self.whole:

            @pl.when(number % 2 != self.place.core)
            def _():
                self.copy(number).start()
        else:
            self.copy(number).start()

    def finish(self):
        if self.whole:
            for n in range(DEVICES // 2):
                self.copy(2 * n + 1 - self.place.core).wait_send()
                self.copy(2 * n + self.place.core).wait_recv()
        else:
            for n in range(self.steps):
                self.copy(n).wait()

        @pl.loop(0, 8)
        def _(n):
            block = (n // 4, (n // 2) % 2, n % 2)

            @pl.loop(0, self.rows // 16)
            def _(strip):
                rest = (pl.ds(strip * 16, 16), slice(None))
                mine = self.partial[(*block, self.place.core, *rest)].astype(F32)
                self.out[(*block, *rest)] = (mine + self.landed[(*block, *rest)].astype(F32)).astype(BF16)


class Norm:
    def __init__(self, place, own, all_of, out, send, recv):
        self.place, self.own, self.all_of, self.out, self.send, self.recv = place, own, all_of, out, send, recv

    def exchange(self):
        me, others = self.place.me, [(self.place.me + k) % DEVICES for k in range(1, DEVICES)]
        copies = [remote(self.own, self.all_of.at[me], self.send.at[k], self.recv.at[me], other) for k, other in enumerate(others)]
        for copy in copies:
            copy.start()
        self.all_of[me] = self.own[...]
        for k, other in enumerate(others):
            remote(self.own, self.all_of.at[other], self.send.at[k], self.recv.at[other], other).wait_recv()
        for copy in copies:
            copy.wait_send()
        total = self.all_of[0]
        for k in range(1, DEVICES):
            total = total + self.all_of[k]
        self.out[...] = total


ANY = pl.BlockSpec(memory_space=pl.ANY)


def once(shape):
    return pl.BlockSpec(shape, lambda i: (0,) * len(shape), pipeline_mode=pl.Buffered(1))


def fused(name, cid, steps, body, ins, in_specs, outs, out_specs, scratch, gathers=(), scatters=(), kept=(), norm_of=(), see=False, prelude=None, pair=None):
    n_in, n_out = len(ins), len(outs)
    ng, ns, nk, nn = len(gathers), len(scatters), len(kept), len(norm_of)
    in_specs, ins, outs, out_specs = list(in_specs), list(ins), list(outs), list(out_specs)
    scratch = list(scratch)
    n_scratch = len(scratch)
    for w, layer, _ in gathers:
        r, c = w.shape[1:]
        ins.append(w)
        in_specs.append(pl.BlockSpec((1, r, c), lambda i, layer=layer: (layer, 0, 0), pipeline_mode=pl.Buffered(1)))
        outs.append(jax.ShapeDtypeStruct((2, 2, 2, 2, r, c), BF16))
        out_specs.append(ANY)
        scratch += [pltpu.SemaphoreType.DMA((10,)), pltpu.SemaphoreType.DMA((10,)), pltpu.SemaphoreType.DMA]
    for d, _ in scatters:
        ins.append(d)
        in_specs.append(ANY)
    for r, c in [d.shape[-2:] for d, _ in scatters] + [k[:2] for k in kept]:
        outs.append(jax.ShapeDtypeStruct((r, c), BF16))
        out_specs.append(pl.BlockSpec((r, c), lambda i: (0, 0), pipeline_mode=pl.Buffered(1)))
    for d, _ in scatters:
        scratch += scatter_scratch(*d.shape[-2:], paired=d.ndim == 5)
    for r, c, whens in kept:
        for _ in whens:
            scratch += scatter_scratch(r, c // len(whens), True)
    for g in norm_of:
        ins.append(g)
        in_specs.append(once(g.shape))
    if pair:
        half = (2, 2, 2, *pair)
        outs.append(jax.ShapeDtypeStruct(half, BF16))
        out_specs.append(once(half))
        scratch += [pltpu.VMEM((2, 2, 2, 2, *pair), BF16), pltpu.VMEM(half, BF16)]
        scratch += [pltpu.SemaphoreType.DMA((steps,)), pltpu.SemaphoreType.DMA((steps,))]
    if nn:
        outs.append(jax.ShapeDtypeStruct((8, 128), F32))
        out_specs.append(once((8, 128)))
        scratch += [pltpu.VMEM((8, 128), F32), pltpu.VMEM((DEVICES, 8, 128), F32)]
        scratch += [pltpu.SemaphoreType.DMA((DEVICES,)), pltpu.SemaphoreType.DMA((DEVICES,))]

    def kernel(*refs):
        refs = list(refs)

        def take(n):
            taken, refs[:n] = refs[:n], []
            return taken

        body_in, own, partial, known = take(n_in), take(ng), take(ns), take(nn)
        body_out, full, mine, sum_out = take(n_out), take(ng), take(ns + nk), take(1 if nn or pair else 0)
        own_scratch = take(n_scratch)
        place = Place()
        exchanges = [(Gather(place, own[g].at[0], full[g], *take(3)), gathers[g][2]) for g in range(ng)]
        for s in range(ns):
            got = take(14)
            exchanges.append((Scatter(place, partial[s], mine[s], got[0], got[1], got[2:11], *got[11:]), scatters[s][1]))
        for (_, c, whens), out in zip(kept, mine[ns:]):
            for k, when in enumerate(whens):
                got, size = take(14), c // len(whens)
                own_scratch.append(got[0])
                piece = out.at[:, pl.ds(k * size, size)]
                exchanges.append((Scatter(place, got[0], piece, None, got[1], got[2:11], *got[11:]), when))
        if pair:
            got = take(4)
            own_scratch.append(got[0])
            twins = Pair(place, steps, sum_out[0], *got)
        if nn:
            norm = Norm(place, *take(1), *take(1), sum_out[0], *take(2))
        step = pl.program_id(0)
        acts = sorted([(at, n, j) for n, (_, when) in enumerate(exchanges) for j, at in enumerate(when)] + [(0.05, -1, 0)] * bool(prelude))

        def due(place_of):
            for at, n, j in acts:
                if int(at) == place_of:
                    if n < 0:
                        prelude(*body_in, *body_out)
                    else:
                        exchanges[n][0].act(j)

        for at in sorted({int(at) for at, _, _ in acts if at < steps} | {0}):

            @pl.when(step == at)
            def _(at=at):
                if at == 0:
                    place.greet(bool(nn))
                due(at)

        body(step, *body_in, *body_out, *own_scratch, *(full if see else ()))

        if pair:
            twins.made(step)
        if nn:

            @pl.when(step == 2)
            def _():
                norm.own[...] = jnp.full((8, 128), sum(squares(ref) for ref in known), F32)

        @pl.when(step == steps - 1)
        def _():
            due(steps)
            if pair:
                twins.finish()
            if nn:
                norm.own[...] += jnp.full((8, 128), sum(squares(ref) for ref in mine), F32)
                norm.exchange()

    return pl.pallas_call(
        kernel,
        grid=(steps,),
        in_specs=in_specs,
        out_specs=out_specs,
        out_shape=outs,
        scratch_shapes=scratch,
        name=name,
        compiler_params=pltpu.CompilerParams(
            dimension_semantics=("arbitrary",), collective_id=cid, has_side_effects=True, vmem_limit_bytes=VMEM_LIMIT
        ),
    )(*ins)


def squares(ref):
    rows, columns = ref.shape

    def strip(s, total):
        part = ref[pl.ds(s * 16, 16), :].astype(F32)
        part = part * part
        return total + sum(part[:, c : c + 128] for c in range(0, columns, 128))

    return jnp.sum(lax.fori_loop(0, rows // 16, strip, jnp.zeros((16, 128), F32)))


def dot(a, b, contract=(1, 0)):
    return lax.dot_general(a, b, (((contract[0],), (contract[1],)), ((), ())), preferred_element_type=F32)


CHUNK = 512


def chunks(tokens, do, unroll=True):
    @pl.loop(0, tokens // CHUNK, unroll=unroll)
    def _(m):
        do(pl.ds(pl.multiple_of(m * CHUNK, CHUNK), CHUNK))


def strips(tokens, do):
    @pl.loop(0, tokens // 64)
    def _(m):
        do(pl.ds(pl.multiple_of(m * 64, 64), 64))


def normed(h):
    wide = h.astype(F32)
    return (wide * lax.rsqrt(jnp.mean(wide**2, -1, keepdims=True) + 1e-6)).astype(BF16)


def normed_back(h, by_a):
    wide, by_a = h.astype(F32), by_a.astype(F32)
    scale = lax.rsqrt(jnp.mean(wide**2, -1, keepdims=True) + 1e-6)
    return (by_a * scale - wide * (scale * scale * scale * jnp.mean(by_a * wide, -1, keepdims=True))).astype(BF16)


def forward_prelude(x, a, *_):
    def do(rows):
        a[rows, :] = normed(x[rows, :])

    strips(x.shape[0], do)


def forward_body(tiles, step, x, a, gate, up, h, a_next, hidden, w, wd, w_sem, wd_sem, g_full, u_full, d_full, *_):
    width = gate.shape[1]

    def copy(t, slot, m):
        columns = pl.ds(pl.multiple_of(t * width, width), width)
        return pltpu.make_async_copy((g_full, u_full)[m].at[:, :, :, :, :, columns], w.at[slot, m], w_sem.at[slot, m])

    @pl.when((step >= 1) & (step <= tiles))
    def _():
        t = step - 1
        slot = t % 2

        @pl.when(t == 0)
        def _():
            for m in range(2):
                copy(t, slot, m).start()

        @pl.when(t + 1 < tiles)
        def _():
            for m in range(2):
                copy(t + 1, 1 - slot, m).start()

        for m in range(2):
            copy(t, slot, m).wait()
        columns = pl.ds(pl.multiple_of(t * width, width), width)

        def do(rows):
            g = dot(a[rows, :], w[slot, 0].reshape(-1, width))
            u = dot(a[rows, :], w[slot, 1].reshape(-1, width))
            gate[rows, :], up[rows, :] = g, u
            hidden[rows, columns] = (g * jax.nn.sigmoid(g) * u).astype(BF16)

        chunks(a.shape[0], do)

    @pl.when(step == tiles + 1)
    def _():
        pltpu.make_async_copy(d_full, wd, wd_sem).start()
        pltpu.make_async_copy(d_full, wd, wd_sem).wait()

    @pl.when(step > tiles)
    def _():
        height = h.shape[0]
        rows = pl.ds(pl.multiple_of((step - tiles - 1) * height, height), height)
        out = dot(hidden[rows, :], wd[...].reshape(-1, wd.shape[-1])).astype(BF16).astype(F32)
        new = (x[rows, :].astype(F32) + out).astype(BF16)
        h[...] = new
        a_next[...] = normed(new)


def forward_last_body(step, a, wg, wu, dy, gate, up, dwd, hidden):
    def do(rows):
        g, u = dot(a[rows, :], wg[...]), dot(a[rows, :], wu[...])
        gate[rows, :], up[rows, :] = g, u
        hidden[rows, :] = (g * jax.nn.sigmoid(g) * u).astype(BF16)

    chunks(a.shape[0], do)
    dwd[...] = dot(hidden[...], dy[...], (0, 0)).astype(BF16)


def through_gate(dy, wd, gate, up, dgate, dup, hidden, rows):
    by_hidden = dot(dy[rows, :], wd[...], (1, 1)).astype(BF16).astype(F32)
    g, u = gate[rows, :], up[rows, :]
    s = jax.nn.sigmoid(g)
    silu = g * s
    dup[rows, :] = (by_hidden * silu).astype(BF16)
    dgate[rows, :] = (by_hidden * u * (s + silu * (1.0 - s))).astype(BF16)
    if hidden is not None:
        hidden[rows, :] = (silu * u).astype(BF16)


def turn(a, at):
    for m in range(a.shape[0] // 256):
        at[:, m * 256 : (m + 1) * 256] = a[m * 256 : (m + 1) * 256, :].T


def back_last_body(step, dy, wd, gate, up, a, dgate, dup, dwu, at, dwg):
    @pl.when(step == 0)
    def _():
        turn(a, at)

    chunks(a.shape[0], lambda rows: through_gate(dy, wd, gate, up, dgate, dup, None, rows))
    width = dgate.shape[1]
    columns = pl.ds(pl.multiple_of(step * width, width), width)
    dwg[:, :, :, :, :, columns] = dot(at[...], dgate[...]).astype(BF16).reshape(*dwg.shape[:5], width)
    dwu[...] = dot(at[...], dup[...]).astype(BF16)


def by_input_body(last, step, dgate, dup, wg, wu, h, dy, by_h, total, ends, sems):
    def copies():
        return [pltpu.make_async_copy(ref, ends.at[n], sems.at[n]) for n, ref in enumerate((h, dy))]

    @pl.when(step == 0)
    def _():
        for copy in copies():
            copy.start()
        total[...] = jnp.zeros_like(total)

    def do(rows):
        total[rows, :] += dot(dgate[rows, :], wg[...], (1, 1)) + dot(dup[rows, :], wu[...], (1, 1))

    chunks(dgate.shape[0], do)

    @pl.when(step == last)
    def _():
        for copy in copies():
            copy.wait()

        def finish(rows):
            by_norm = normed_back(ends[0, rows, :], total[rows, :].astype(BF16))
            by_h[rows, :] = (ends[1, rows, :].astype(F32) + by_norm.astype(F32)).astype(BF16)

        strips(dgate.shape[0], finish)


def back_first_body(step, dy, wd, gate, up, dgate, dup, hidden, dwd):
    chunks(dy.shape[0], lambda rows: through_gate(dy, wd, gate, up, dgate, dup, hidden, rows))
    block = (step // 8, (step // 4) % 2, (step // 2) % 2, step % 2)
    dwd[(*block, slice(None), slice(None))] = dot(hidden[...], dy[...], (0, 0)).astype(BF16)


def weights_body(half, step, a, dgate, dup, at, *dws):
    @pl.when(step == 0)
    def _():
        turn(a, at)

    steps = 2 * half // len(dws)
    for number, dw in enumerate(dws):
        d = dgate if 2 * number < len(dws) else dup

        @pl.when(step // steps == number)
        def _(d=d, dw=dw, number=number):
            width = d.shape[1]
            columns = pl.ds(pl.multiple_of((step - number * steps) * width, width), width)
            dw[:, :, :, :, :, columns] = dot(at[...], d[...]).astype(BF16).reshape(*dw.shape[:5], width)


def solution(mesh):
    def step(x, dy, *arrays):
        weights, m, v = (arrays[i : i + 3] for i in (0, 3, 6))
        w_gate, w_up, w_down = weights
        x, dy = x[0], dy[0]
        tokens, d = x.shape
        ff = w_gate.shape[-1]
        tile = 256
        n = ff // tile

        def of(shape, dtype=BF16):
            return jax.ShapeDtypeStruct(shape, dtype)

        def columns(rows, width=tile):
            return pl.BlockSpec((rows, width), lambda i: (0, i))

        def rows_of(width, height=tile):
            return pl.BlockSpec((height, width), lambda i: (i, 0))

        def flat(full):
            return full.reshape(-1, full.shape[-1])

        def blocks(dw):
            return dw.reshape(2, 2, 2, 2, dw.shape[0] // 16, dw.shape[1])

        here = once((tokens, d))
        states = [of((tokens, ff), F32)] * 2
        halves = [of((tokens, ff))] * 2
        height = 256
        parts = tokens // height
        last = 1 + n + parts

        def tiles_of(i):
            return (0, jnp.clip(i - 1, 0, n - 1))

        def parts_of(i):
            return (jnp.clip(i - 1 - n, 0, parts - 1), 0)

        a0, gate0, up0, h1, a1, _, _, d0, g1, u1 = fused(
            "forward0", 2, last, functools.partial(forward_body, n), [x], [here],
            [of((tokens, d)), *states, of((tokens, d)), of((tokens, d))],
            [here, *[pl.BlockSpec((tokens, tile), tiles_of)] * 2, *[pl.BlockSpec((height, d), parts_of)] * 2],
            [
                pltpu.VMEM((tokens, ff), BF16), pltpu.VMEM((2, 2, 2, 2, 2, 2, d // DEVICES, tile), BF16),
                pltpu.VMEM((2, 2, 2, 2, ff // DEVICES, d), BF16), pltpu.SemaphoreType.DMA((2, 2)), pltpu.SemaphoreType.DMA,
            ],
            gathers=[
                (w_gate, 0, (0, 0.10, 0.20, 0.30, 0.50)),
                (w_up, 0, (0, 0.11, 0.21, 0.40, 0.51)),
                (w_down, 0, (0.22, 0.60, 6, 14, n + 1)),
                (w_gate, 1, (0.23, 0.61, 12, n + 7, last + 0.4)),
                (w_up, 1, (0.24, 6.5, n + 1.5, last + 0.1, last + 0.5)),
            ],
            see=True, prelude=forward_prelude,
        )
        d0 = flat(d0)
        g1, u1 = map(flat, (g1, u1))
        gate1, up1, dwd1, d1 = fused(
            "forward1", 3, n, forward_last_body,
            [a1, g1, u1, dy], [here, columns(d), columns(d), here],
            [*states, of((ff, d))], [columns(tokens), columns(tokens), rows_of(d)],
            [pltpu.VMEM((tokens, tile), BF16)],
            gathers=[(w_down, 1, (0, 2, 5, 10, 14))],
        )
        d1 = flat(d1)
        dgate1, dup1, dwu1, sd1, dwg1 = fused(
            "back1", 4, n, back_last_body,
            [dy, d1, gate1, up1, a1], [here, rows_of(d), columns(tokens), columns(tokens), here],
            [*halves, of((d, ff))], [columns(tokens), columns(tokens), columns(d)],
            [pltpu.VMEM((d, tokens), BF16)],
            scatters=[(blocks(dwd1), (0, 3, 8, 11, 14))],
            pair=(d // DEVICES, ff),
        )
        wide = 512
        by_h, sg1 = fused(
            "by_input1", 5, ff // wide, functools.partial(by_input_body, ff // wide - 1),
            [dgate1, dup1, g1, u1, h1, dy],
            [*[columns(tokens, wide)] * 2, *[columns(d, wide)] * 2, ANY, ANY],
            [of((tokens, d))], [here],
            [pltpu.VMEM((tokens, d), F32), pltpu.VMEM((2, tokens, d), BF16), pltpu.SemaphoreType.DMA((2,))],
            scatters=[(dwg1, (0, 0.1, 4, 6, 8))],
        )
        dgate0, dup0, su1, dwd0 = fused(
            "back0", 6, n, back_first_body,
            [by_h, d0, gate0, up0], [here, rows_of(d), columns(tokens), columns(tokens)],
            halves, [columns(tokens), columns(tokens)],
            [pltpu.VMEM((tokens, tile), BF16)],
            scatters=[(blocks(dwu1), (0, 3, 9, 12, 15))],
            pair=(ff // DEVICES, d),
        )
        end = 2 * n
        sd0, sg0, su0, squares_sum = fused(
            "finish", 7, end, functools.partial(weights_body, n),
            [a0, dgate0, dup0],
            [
                here,
                pl.BlockSpec((tokens, tile), lambda i: (0, jnp.minimum(i, n - 1))),
                pl.BlockSpec((tokens, tile), lambda i: (0, jnp.maximum(i - n, 0))),
            ],
            [], [], [pltpu.VMEM((d, tokens), BF16)],
            scatters=[(dwd0, (0, 0.1, 14, 20.5, 29))],
            kept=[
                (d // DEVICES, ff, [(8, 14.5, 27, end + 0.15, end + 0.35), (16, 22, end + 0.05, end + 0.25, end + 0.45)]),
                (d // DEVICES, ff, [(24, 30, end + 0.2, end + 0.4, end + 0.55), (end, end + 0.1, end + 0.3, end + 0.5, end + 0.6)]),
            ],
            norm_of=[sg1, su1, sd1],
        )
        gradients = [jnp.stack(pair).astype(F32) for pair in ((sg0, sg1), (su0, su1), (sd0, sd1))]
        gradients = clipped(gradients, squares_sum[0, 0], DEVICES * sum(g.size for g in gradients))
        new = [adamw(w.astype(F32), m, v, g) for w, m, v, g in zip(weights, m, v, gradients, strict=True)]
        return tuple(one[which] for which in range(3) for one in new)

    states, cut = P(("rep", "dp"), None, None), P(None, "dp", None)
    return jax.shard_map(
        step,
        mesh=mesh,
        in_specs=(states, states) + (cut,) * 9,
        out_specs=(P("rep", "dp", None),) * 9,
        check_vma=False,
    )
```

```python
import functools

import jax
import jax.numpy as jnp
from jax import lax
from jax.experimental import pallas as pl
from jax.experimental.pallas import tpu as pltpu
from jax.sharding import PartitionSpec as P

F32, BF16 = jnp.float32, jnp.bfloat16
NAMES = ("w_gate", "w_up", "w_down")
BITS = (8, 4, 2)
DEVICES = 16
VMEM_LIMIT = 67_000_000


def adamw(w, m, v, g):
    m = 0.9 * m + 0.1 * g
    v = 0.95 * v + 0.05 * g * g
    step = m * lax.rsqrt(v + 1e-8) + 0.1 * w
    return (w - 0.02 * step).astype(BF16), m, v


def clipped(gradients, sum_of_squares, count):
    factor = jnp.minimum(1.0, 0.5 * lax.rsqrt(sum_of_squares / count + 1e-30))
    return [g * factor for g in gradients]


def thirds(columns):
    tiles, start, out = columns // 128, 0, []
    for k in range(3):
        size = 128 * (tiles // 3 + (k < tiles % 3))
        out.append((start, size))
        start += size
    return out


class Place:
    def __init__(self):
        me = self.me = lax.axis_index("dp")
        self.core = me % 2
        self.at = (me // 8, (me // 4) % 2, (me // 2) % 2)
        self.near = tuple(me + bit * (1 - 2 * v) for bit, v in zip(BITS, self.at))
        self.twin = me + 1 - 2 * self.core

    def greet(self, everyone):
        barrier = pltpu.get_barrier_semaphore()
        others = [(self.me + k) % DEVICES for k in range(1, DEVICES)] if everyone else [*self.near, self.twin]
        for other in others:
            pl.semaphore_signal(barrier, inc=1, device_id={"dp": other}, device_id_type=pl.DeviceIdType.MESH)
        pl.semaphore_wait(barrier, len(others))


def remote(src, dst, send, recv, device):
    return pltpu.make_async_remote_copy(
        src_ref=src, dst_ref=dst, send_sem=send, recv_sem=recv, device_id={"dp": device}, device_id_type=pl.DeviceIdType.MESH
    )


class Gather:
    def __init__(self, place, own, full, send, recv, here):
        self.place, self.own, self.full, self.send, self.recv, self.here = place, own, full, send, recv, here
        self.cuts = thirds(own.shape[-1])

    def local(self):
        x, y, z = self.place.at
        return pltpu.make_async_copy(self.own, self.full.at[x, y, z, self.place.core], self.here)

    def copy(self, stage, k):
        order = [(k + j) % 3 for j in range(3)]
        at = list(self.place.at)
        for d in order[:stage]:
            at[d] = slice(None)
        columns = pl.ds(*self.cuts[k])
        region = self.full.at[(*at, self.place.core, slice(None), columns)]
        src = region if stage else self.own.at[:, columns]
        n = 3 * stage + k
        return remote(src, region, self.send.at[n], self.recv.at[n], self.place.near[order[stage]])

    def across(self):
        region = self.full.at[:, :, :, self.place.core]
        return remote(region, region, self.send.at[9], self.recv.at[9], self.place.twin)

    def act(self, j):
        if j == 0:
            self.local().start()
            for k in range(3):
                self.copy(0, k).start()
        elif j in (1, 2):
            if j == 1:
                self.local().wait()
            for k in range(3):
                self.copy(j - 1, k).wait_recv()
                self.copy(j, k).start()
        elif j == 3:
            for k in range(3):
                self.copy(2, k).wait_recv()
            self.across().start()
        else:
            self.across().wait_recv()
            for stage in range(3):
                for k in range(3):
                    self.copy(stage, k).wait_send()
            self.across().wait_send()


class Scatter:
    def __init__(self, place, partial, out, total, first, landed, send, recv, here):
        self.place, self.partial, self.out, self.total, self.first = place, partial, out, total, first
        self.landed, self.send, self.recv, self.here = landed, send, recv, here
        self.rows, self.columns = partial.shape[-2:]
        self.cuts = thirds(self.columns)
        self.strip = 16
        self.kept, self.paired = total is None, len(partial.shape) == 5
        self.sums, self.half = (partial, (place.core,)) if self.kept else (total, ())

    def load(self):
        mine = self.partial if self.paired else self.partial.at[:, :, :, self.place.core]
        return pltpu.make_async_copy(mine, self.total, self.here)

    def across(self):
        return remote(self.partial.at[:, :, :, 1 - self.place.core], self.first, self.send.at[9], self.recv.at[9], self.place.twin)

    def where(self, stage, k, keep):
        order = [(k + j) % 3 for j in range(3)]
        at = [slice(None)] * 3
        for d in order[:stage]:
            at[d] = self.place.at[d]
        d = order[stage]
        at[d] = self.place.at[d] if keep else 1 - self.place.at[d]
        return at, d

    def copy(self, stage, k):
        at, d = self.where(stage, k, False)
        n = 3 * stage + k
        src = self.sums.at[(*at, *self.half, slice(None), pl.ds(*self.cuts[k]))]
        return remote(src, self.landed[n], self.send.at[n], self.recv.at[n], self.place.near[d])

    def add_first(self):
        @pl.loop(0, 8)
        def _(block):
            at = (block // 4, (block // 2) % 2, block % 2)

            @pl.loop(0, self.rows // self.strip)
            def _(strip):
                rest = (pl.ds(strip * self.strip, self.strip), slice(None))
                to = (*at, *self.half, *rest)
                self.sums[to] = (self.sums[to].astype(F32) + self.first[(*at, *rest)].astype(F32)).astype(BF16)

    def add(self, stage, k):
        at, _ = self.where(stage, k, True)
        landed, free = self.landed[3 * stage + k], [d for d in range(3) if isinstance(at[d], slice)]
        columns = pl.ds(*self.cuts[k])
        for number in range(2 ** len(free)):
            bits = [(number >> b) & 1 for b in reversed(range(len(free)))]
            spot = list(at)
            for d, bit in zip(free, bits):
                spot[d] = bit

            @pl.loop(0, self.rows // self.strip)
            def _(strip, spot=spot, bits=bits):
                rows = pl.ds(strip * self.strip, self.strip)
                to = (*spot, *self.half, rows, columns)
                value = (self.sums[to].astype(F32) + landed[(*bits, rows, slice(None))].astype(F32)).astype(BF16)
                if stage < 2:
                    self.sums[to] = value
                else:
                    self.out[rows, columns] = value

    def act(self, j):
        if j == 0:
            if not self.paired:
                self.across().start()
            if not self.kept:
                self.load().start()
        elif j == 1:
            if not self.kept:
                self.load().wait()
            if not self.paired:
                self.across().wait_recv()
                self.add_first()
            for k in range(3):
                self.copy(0, k).start()
        elif j in (2, 3):
            for k in range(3):
                self.copy(j - 2, k).wait_recv()
                self.add(j - 2, k)
                self.copy(j - 1, k).start()
        else:
            for k in range(3):
                self.copy(2, k).wait_recv()
                self.add(2, k)
            for stage in range(3):
                for k in range(3):
                    self.copy(stage, k).wait_send()
            if not self.paired:
                self.across().wait_send()


def scatter_scratch(rows, columns, kept=False, paired=False):
    landed = [pltpu.VMEM((2,) * (2 - stage) + (rows, size), BF16) for stage in range(3) for _, size in thirds(columns)]
    half = pltpu.VMEM((2, 2, 2, rows, columns), BF16)
    mine = pltpu.VMEM((2, 2, 2, 2, rows, columns), BF16) if kept else half
    return [mine, pltpu.VMEM((8, 128), BF16) if paired else half, *landed, pltpu.SemaphoreType.DMA((10,)), pltpu.SemaphoreType.DMA((10,)), pltpu.SemaphoreType.DMA]


class Pair:
    def __init__(self, place, steps, out, partial, landed, send, recv):
        self.place, self.out, self.partial, self.landed, self.send, self.recv = place, out, partial, landed, send, recv
        self.rows, self.columns = partial.shape[-2:]
        self.steps, self.whole = steps, steps == DEVICES and self.rows * DEVICES > self.columns

    def copy(self, number):
        if self.whole:
            block = (number // 8, (number // 4) % 2, (number // 2) % 2)
            src, dst = self.partial.at[(*block, number % 2)], self.landed.at[block]
        else:
            width = self.columns // self.steps
            columns = pl.ds(pl.multiple_of(number * width, width), width)
            src = self.partial.at[:, :, :, 1 - self.place.core, :, columns]
            dst = self.landed.at[:, :, :, :, columns]
        return remote(src, dst, self.send.at[number], self.recv.at[number], self.place.twin)

    def made(self, number):
        if self.whole:

            @pl.when(number % 2 != self.place.core)
            def _():
                self.copy(number).start()
        else:
            self.copy(number).start()

    def finish(self):
        if self.whole:
            for n in range(DEVICES // 2):
                self.copy(2 * n + 1 - self.place.core).wait_send()
                self.copy(2 * n + self.place.core).wait_recv()
        else:
            for n in range(self.steps):
                self.copy(n).wait()

        @pl.loop(0, 8)
        def _(n):
            block = (n // 4, (n // 2) % 2, n % 2)

            @pl.loop(0, self.rows // 16)
            def _(strip):
                rest = (pl.ds(strip * 16, 16), slice(None))
                mine = self.partial[(*block, self.place.core, *rest)].astype(F32)
                self.out[(*block, *rest)] = (mine + self.landed[(*block, *rest)].astype(F32)).astype(BF16)


class Norm:
    def __init__(self, place, own, all_of, out, send, recv):
        self.place, self.own, self.all_of, self.out, self.send, self.recv = place, own, all_of, out, send, recv

    def exchange(self):
        me, others = self.place.me, [(self.place.me + k) % DEVICES for k in range(1, DEVICES)]
        copies = [remote(self.own, self.all_of.at[me], self.send.at[k], self.recv.at[me], other) for k, other in enumerate(others)]
        for copy in copies:
            copy.start()
        self.all_of[me] = self.own[...]
        for k, other in enumerate(others):
            remote(self.own, self.all_of.at[other], self.send.at[k], self.recv.at[other], other).wait_recv()
        for copy in copies:
            copy.wait_send()
        total = self.all_of[0]
        for k in range(1, DEVICES):
            total = total + self.all_of[k]
        self.out[...] = total


ANY = pl.BlockSpec(memory_space=pl.ANY)


def once(shape):
    return pl.BlockSpec(shape, lambda i: (0,) * len(shape), pipeline_mode=pl.Buffered(1))


def fused(name, cid, steps, body, ins, in_specs, outs, out_specs, scratch, gathers=(), scatters=(), kept=(), norm_of=(), see=False, prelude=None, pair=None):
    n_in, n_out = len(ins), len(outs)
    ng, ns, nk, nn = len(gathers), len(scatters), len(kept), len(norm_of)
    in_specs, ins, outs, out_specs = list(in_specs), list(ins), list(outs), list(out_specs)
    scratch = list(scratch)
    n_scratch = len(scratch)
    for w, layer, _ in gathers:
        r, c = w.shape[1:]
        ins.append(w)
        in_specs.append(pl.BlockSpec((1, r, c), lambda i, layer=layer: (layer, 0, 0), pipeline_mode=pl.Buffered(1)))
        outs.append(jax.ShapeDtypeStruct((2, 2, 2, 2, r, c), BF16))
        out_specs.append(ANY)
        scratch += [pltpu.SemaphoreType.DMA((10,)), pltpu.SemaphoreType.DMA((10,)), pltpu.SemaphoreType.DMA]
    for d, _ in scatters:
        ins.append(d)
        in_specs.append(ANY)
    for r, c in [d.shape[-2:] for d, _ in scatters] + [k[:2] for k in kept]:
        outs.append(jax.ShapeDtypeStruct((r, c), BF16))
        out_specs.append(pl.BlockSpec((r, c), lambda i: (0, 0), pipeline_mode=pl.Buffered(1)))
    for d, _ in scatters:
        scratch += scatter_scratch(*d.shape[-2:], paired=d.ndim == 5)
    for r, c, whens in kept:
        for _ in whens:
            scratch += scatter_scratch(r, c // len(whens), True)
    for g in norm_of:
        ins.append(g)
        in_specs.append(once(g.shape))
    if pair:
        half = (2, 2, 2, *pair)
        outs.append(jax.ShapeDtypeStruct(half, BF16))
        out_specs.append(once(half))
        scratch += [pltpu.VMEM((2, 2, 2, 2, *pair), BF16), pltpu.VMEM(half, BF16)]
        scratch += [pltpu.SemaphoreType.DMA((steps,)), pltpu.SemaphoreType.DMA((steps,))]
    if nn:
        outs.append(jax.ShapeDtypeStruct((8, 128), F32))
        out_specs.append(once((8, 128)))
        scratch += [pltpu.VMEM((8, 128), F32), pltpu.VMEM((DEVICES, 8, 128), F32)]
        scratch += [pltpu.SemaphoreType.DMA((DEVICES,)), pltpu.SemaphoreType.DMA((DEVICES,))]

    def kernel(*refs):
        refs = list(refs)

        def take(n):
            taken, refs[:n] = refs[:n], []
            return taken

        body_in, own, partial, known = take(n_in), take(ng), take(ns), take(nn)
        body_out, full, mine, sum_out = take(n_out), take(ng), take(ns + nk), take(1 if nn or pair else 0)
        own_scratch = take(n_scratch)
        place = Place()
        exchanges = [(Gather(place, own[g].at[0], full[g], *take(3)), gathers[g][2]) for g in range(ng)]
        for s in range(ns):
            got = take(14)
            exchanges.append((Scatter(place, partial[s], mine[s], got[0], got[1], got[2:11], *got[11:]), scatters[s][1]))
        for (_, c, whens), out in zip(kept, mine[ns:]):
            for k, when in enumerate(whens):
                got, size = take(14), c // len(whens)
                own_scratch.append(got[0])
                piece = out.at[:, pl.ds(k * size, size)]
                exchanges.append((Scatter(place, got[0], piece, None, got[1], got[2:11], *got[11:]), when))
        if pair:
            got = take(4)
            own_scratch.append(got[0])
            twins = Pair(place, steps, sum_out[0], *got)
        if nn:
            norm = Norm(place, *take(1), *take(1), sum_out[0], *take(2))
        step = pl.program_id(0)
        acts = sorted([(at, n, j) for n, (_, when) in enumerate(exchanges) for j, at in enumerate(when)] + [(0.05, -1, 0)] * bool(prelude))

        def due(place_of):
            for at, n, j in acts:
                if int(at) == place_of:
                    if n < 0:
                        prelude(*body_in, *body_out)
                    else:
                        exchanges[n][0].act(j)

        for at in sorted({int(at) for at, _, _ in acts if at < steps} | {0}):

            @pl.when(step == at)
            def _(at=at):
                if at == 0:
                    place.greet(bool(nn))
                due(at)

        body(step, *body_in, *body_out, *own_scratch, *(full if see else ()))

        if pair:
            twins.made(step)
        if nn:

            @pl.when(step == 2)
            def _():
                norm.own[...] = jnp.full((8, 128), sum(squares(ref) for ref in known), F32)

        @pl.when(step == steps - 1)
        def _():
            due(steps)
            if pair:
                twins.finish()
            if nn:
                norm.own[...] += jnp.full((8, 128), sum(squares(ref) for ref in mine), F32)
                norm.exchange()

    return pl.pallas_call(
        kernel,
        grid=(steps,),
        in_specs=in_specs,
        out_specs=out_specs,
        out_shape=outs,
        scratch_shapes=scratch,
        name=name,
        compiler_params=pltpu.CompilerParams(
            dimension_semantics=("arbitrary",), collective_id=cid, has_side_effects=True, vmem_limit_bytes=VMEM_LIMIT
        ),
    )(*ins)


def squares(ref):
    rows, columns = ref.shape

    def strip(s, total):
        part = ref[pl.ds(s * 16, 16), :].astype(F32)
        part = part * part
        return total + sum(part[:, c : c + 128] for c in range(0, columns, 128))

    return jnp.sum(lax.fori_loop(0, rows // 16, strip, jnp.zeros((16, 128), F32)))


def dot(a, b, contract=(1, 0)):
    return lax.dot_general(a, b, (((contract[0],), (contract[1],)), ((), ())), preferred_element_type=F32)


CHUNK = 512


def chunks(tokens, do, unroll=True):
    @pl.loop(0, tokens // CHUNK, unroll=unroll)
    def _(m):
        do(pl.ds(pl.multiple_of(m * CHUNK, CHUNK), CHUNK))


def strips(tokens, do):
    @pl.loop(0, tokens // 64)
    def _(m):
        do(pl.ds(pl.multiple_of(m * 64, 64), 64))


def normed(h):
    wide = h.astype(F32)
    return (wide * lax.rsqrt(jnp.mean(wide**2, -1, keepdims=True) + 1e-6)).astype(BF16)


def normed_back(h, by_a):
    wide, by_a = h.astype(F32), by_a.astype(F32)
    scale = lax.rsqrt(jnp.mean(wide**2, -1, keepdims=True) + 1e-6)
    return (by_a * scale - wide * (scale * scale * scale * jnp.mean(by_a * wide, -1, keepdims=True))).astype(BF16)


def forward_prelude(x, a, *_):
    def do(rows):
        a[rows, :] = normed(x[rows, :])

    strips(x.shape[0], do)


def forward_body(tiles, step, x, a, gate, up, h, a_next, hidden, w, wd, w_sem, wd_sem, g_full, u_full, d_full, *_):
    width = gate.shape[1]

    def copy(t, slot, m):
        columns = pl.ds(pl.multiple_of(t * width, width), width)
        return pltpu.make_async_copy((g_full, u_full)[m].at[:, :, :, :, :, columns], w.at[slot, m], w_sem.at[slot, m])

    @pl.when((step >= 1) & (step <= tiles))
    def _():
        t = step - 1
        slot = t % 2

        @pl.when(t == 0)
        def _():
            for m in range(2):
                copy(t, slot, m).start()

        @pl.when(t + 1 < tiles)
        def _():
            for m in range(2):
                copy(t + 1, 1 - slot, m).start()

        for m in range(2):
            copy(t, slot, m).wait()
        columns = pl.ds(pl.multiple_of(t * width, width), width)

        def do(rows):
            g = dot(a[rows, :], w[slot, 0].reshape(-1, width))
            u = dot(a[rows, :], w[slot, 1].reshape(-1, width))
            gate[rows, :], up[rows, :] = g, u
            hidden[rows, columns] = (g * jax.nn.sigmoid(g) * u).astype(BF16)

        chunks(a.shape[0], do)

    @pl.when(step == tiles + 1)
    def _():
        pltpu.make_async_copy(d_full, wd, wd_sem).start()
        pltpu.make_async_copy(d_full, wd, wd_sem).wait()

    @pl.when(step > tiles)
    def _():
        height = h.shape[0]
        rows = pl.ds(pl.multiple_of((step - tiles - 1) * height, height), height)
        out = dot(hidden[rows, :], wd[...].reshape(-1, wd.shape[-1])).astype(BF16).astype(F32)
        new = (x[rows, :].astype(F32) + out).astype(BF16)
        h[...] = new
        a_next[...] = normed(new)


def forward_last_body(step, a, wg, wu, dy, gate, up, dwd, hidden):
    def do(rows):
        g, u = dot(a[rows, :], wg[...]), dot(a[rows, :], wu[...])
        gate[rows, :], up[rows, :] = g, u
        hidden[rows, :] = (g * jax.nn.sigmoid(g) * u).astype(BF16)

    chunks(a.shape[0], do)
    dwd[...] = dot(hidden[...], dy[...], (0, 0)).astype(BF16)


def through_gate(dy, wd, gate, up, dgate, dup, hidden, rows):
    by_hidden = dot(dy[rows, :], wd[...], (1, 1)).astype(BF16).astype(F32)
    g, u = gate[rows, :], up[rows, :]
    s = jax.nn.sigmoid(g)
    silu = g * s
    dup[rows, :] = (by_hidden * silu).astype(BF16)
    dgate[rows, :] = (by_hidden * u * (s + silu * (1.0 - s))).astype(BF16)
    if hidden is not None:
        hidden[rows, :] = (silu * u).astype(BF16)


def turn(a, at):
    for m in range(a.shape[0] // 256):
        at[:, m * 256 : (m + 1) * 256] = a[m * 256 : (m + 1) * 256, :].T


def back_last_body(step, dy, wd, gate, up, a, dgate, dup, dwu, at, dwg):
    @pl.when(step == 0)
    def _():
        turn(a, at)

    chunks(a.shape[0], lambda rows: through_gate(dy, wd, gate, up, dgate, dup, None, rows))
    width = dgate.shape[1]
    columns = pl.ds(pl.multiple_of(step * width, width), width)
    dwg[:, :, :, :, :, columns] = dot(at[...], dgate[...]).astype(BF16).reshape(*dwg.shape[:5], width)
    dwu[...] = dot(at[...], dup[...]).astype(BF16)


def by_input_body(last, step, dgate, dup, wg, wu, h, dy, by_h, total, ends, sems):
    def copies():
        return [pltpu.make_async_copy(ref, ends.at[n], sems.at[n]) for n, ref in enumerate((h, dy))]

    @pl.when(step == 0)
    def _():
        for copy in copies():
            copy.start()
        total[...] = jnp.zeros_like(total)

    def do(rows):
        total[rows, :] += dot(dgate[rows, :], wg[...], (1, 1)) + dot(dup[rows, :], wu[...], (1, 1))

    chunks(dgate.shape[0], do)

    @pl.when(step == last)
    def _():
        for copy in copies():
            copy.wait()

        def finish(rows):
            by_norm = normed_back(ends[0, rows, :], total[rows, :].astype(BF16))
            by_h[rows, :] = (ends[1, rows, :].astype(F32) + by_norm.astype(F32)).astype(BF16)

        strips(dgate.shape[0], finish)


def back_first_body(step, dy, wd, gate, up, dgate, dup, hidden, dwd):
    chunks(dy.shape[0], lambda rows: through_gate(dy, wd, gate, up, dgate, dup, hidden, rows))
    block = (step // 8, (step // 4) % 2, (step // 2) % 2, step % 2)
    dwd[(*block, slice(None), slice(None))] = dot(hidden[...], dy[...], (0, 0)).astype(BF16)


def weights_body(half, step, a, dgate, dup, at, *dws):
    @pl.when(step == 0)
    def _():
        turn(a, at)

    steps = 2 * half // len(dws)
    for number, dw in enumerate(dws):
        d = dgate if 2 * number < len(dws) else dup

        @pl.when(step // steps == number)
        def _(d=d, dw=dw, number=number):
            width = d.shape[1]
            columns = pl.ds(pl.multiple_of((step - number * steps) * width, width), width)
            dw[:, :, :, :, :, columns] = dot(at[...], d[...]).astype(BF16).reshape(*dw.shape[:5], width)


def solution(mesh):
    def step(x, dy, *arrays):
        weights, m, v = (arrays[i : i + 3] for i in (0, 3, 6))
        w_gate, w_up, w_down = weights
        x, dy = x[0], dy[0]
        tokens, d = x.shape
        ff = w_gate.shape[-1]
        tile = 256
        n = ff // tile

        def of(shape, dtype=BF16):
            return jax.ShapeDtypeStruct(shape, dtype)

        def columns(rows, width=tile):
            return pl.BlockSpec((rows, width), lambda i: (0, i))

        def rows_of(width, height=tile):
            return pl.BlockSpec((height, width), lambda i: (i, 0))

        def flat(full):
            return full.reshape(-1, full.shape[-1])

        def blocks(dw):
            return dw.reshape(2, 2, 2, 2, dw.shape[0] // 16, dw.shape[1])

        here = once((tokens, d))
        states = [of((tokens, ff), F32)] * 2
        halves = [of((tokens, ff))] * 2
        height = 256
        parts = tokens // height
        last = 1 + n + parts

        def tiles_of(i):
            return (0, jnp.clip(i - 1, 0, n - 1))

        def parts_of(i):
            return (jnp.clip(i - 1 - n, 0, parts - 1), 0)

        a0, gate0, up0, h1, a1, _, _, d0, g1, u1 = fused(
            "forward0", 2, last, functools.partial(forward_body, n), [x], [here],
            [of((tokens, d)), *states, of((tokens, d)), of((tokens, d))],
            [here, *[pl.BlockSpec((tokens, tile), tiles_of)] * 2, *[pl.BlockSpec((height, d), parts_of)] * 2],
            [
                pltpu.VMEM((tokens, ff), BF16), pltpu.VMEM((2, 2, 2, 2, 2, 2, d // DEVICES, tile), BF16),
                pltpu.VMEM((2, 2, 2, 2, ff // DEVICES, d), BF16), pltpu.SemaphoreType.DMA((2, 2)), pltpu.SemaphoreType.DMA,
            ],
            gathers=[
                (w_gate, 0, (0, 0.10, 0.20, 0.30, 0.50)),
                (w_up, 0, (0, 0.11, 0.21, 0.40, 0.51)),
                (w_down, 0, (0.22, 0.60, 6, 14, n + 1)),
                (w_gate, 1, (0.23, 0.61, 12, n + 7, last + 0.4)),
                (w_up, 1, (0.24, 6.5, n + 1.5, last + 0.1, last + 0.5)),
            ],
            see=True, prelude=forward_prelude,
        )
        d0 = flat(d0)
        g1, u1 = map(flat, (g1, u1))
        gate1, up1, dwd1, d1 = fused(
            "forward1", 3, n, forward_last_body,
            [a1, g1, u1, dy], [here, columns(d), columns(d), here],
            [*states, of((ff, d))], [columns(tokens), columns(tokens), rows_of(d)],
            [pltpu.VMEM((tokens, tile), BF16)],
            gathers=[(w_down, 1, (0, 2, 5, 10, 14))],
        )
        d1 = flat(d1)
        dgate1, dup1, dwu1, sd1, dwg1 = fused(
            "back1", 4, n, back_last_body,
            [dy, d1, gate1, up1, a1], [here, rows_of(d), columns(tokens), columns(tokens), here],
            [*halves, of((d, ff))], [columns(tokens), columns(tokens), columns(d)],
            [pltpu.VMEM((d, tokens), BF16)],
            scatters=[(blocks(dwd1), (0, 3, 8, 11, 14))],
            pair=(d // DEVICES, ff),
        )
        wide = 512
        by_h, sg1 = fused(
            "by_input1", 5, ff // wide, functools.partial(by_input_body, ff // wide - 1),
            [dgate1, dup1, g1, u1, h1, dy],
            [*[columns(tokens, wide)] * 2, *[columns(d, wide)] * 2, ANY, ANY],
            [of((tokens, d))], [here],
            [pltpu.VMEM((tokens, d), F32), pltpu.VMEM((2, tokens, d), BF16), pltpu.SemaphoreType.DMA((2,))],
            scatters=[(dwg1, (0, 0.1, 4, 6, 8))],
        )
        dgate0, dup0, su1, dwd0 = fused(
            "back0", 6, n, back_first_body,
            [by_h, d0, gate0, up0], [here, rows_of(d), columns(tokens), columns(tokens)],
            halves, [columns(tokens), columns(tokens)],
            [pltpu.VMEM((tokens, tile), BF16)],
            scatters=[(blocks(dwu1), (0, 3, 9, 12, 15))],
            pair=(ff // DEVICES, d),
        )
        end = 2 * n
        sd0, sg0, su0, squares_sum = fused(
            "finish", 7, end, functools.partial(weights_body, n),
            [a0, dgate0, dup0],
            [
                here,
                pl.BlockSpec((tokens, tile), lambda i: (0, jnp.minimum(i, n - 1))),
                pl.BlockSpec((tokens, tile), lambda i: (0, jnp.maximum(i - n, 0))),
            ],
            [], [], [pltpu.VMEM((d, tokens), BF16)],
            scatters=[(dwd0, (0, 0.1, 13.5, 19.5, 27))],
            kept=[
                (d // DEVICES, ff, [(8, 13.5, 25, 30, end + 0.35), (16, 21, end + 0.05, end + 0.25, end + 0.45)]),
                (d // DEVICES, ff, [(24, 29, end + 0.2, end + 0.4, end + 0.55), (end, end + 0.1, end + 0.3, end + 0.5, end + 0.6)]),
            ],
            norm_of=[sg1, su1, sd1],
        )
        gradients = [jnp.stack(pair).astype(F32) for pair in ((sg0, sg1), (su0, su1), (sd0, sd1))]
        gradients = clipped(gradients, squares_sum[0, 0], DEVICES * sum(g.size for g in gradients))
        new = [adamw(w.astype(F32), m, v, g) for w, m, v, g in zip(weights, m, v, gradients, strict=True)]
        return tuple(one[which] for which in range(3) for one in new)

    states, cut = P(("rep", "dp"), None, None), P(None, "dp", None)
    return jax.shard_map(
        step,
        mesh=mesh,
        in_specs=(states, states) + (cut,) * 9,
        out_specs=(P("rep", "dp", None),) * 9,
        check_vma=False,
    )
```
